32 devices in a mesh: grp: 2 (over x), tm: 16 (over z, y, core).
Axes of the slice: x: 2, y: 2, z: 4, core: 2. Of those that a mesh axis runs over, the one named last changes fastest.
Arguments:
- video_features: bfloat16 [32, 24, 8, 256], P('tm', 'grp'), parts along dimension 1, may hold values from -6 to 6
- cotangent: bfloat16 [32, 24, 8, 256], P('tm', 'grp'), parts along dimension 1, may hold values from -6 to 6
- encoder_weight: bfloat16 [6912, 256], replicated, may hold values from -0.078125 to 0.078125
- down_weight: bfloat16 [2048, 256], replicated, may hold values from -0.125 to 0.125
- coarse_weight: bfloat16 [768, 256], replicated, may hold values from -0.21875 to 0.21875
- up_weight: bfloat16 [256, 2048], replicated, may hold values from -0.375 to 0.375
- decoder_weight: bfloat16 [6912, 256], replicated, may hold values from -0.078125 to 0.078125
- levels: int32 [256], replicated, may hold values from 3 to 8
Outputs:
- video_grad: bfloat16 [32, 24, 8, 256], P('tm', 'grp'), parts along dimension 1
- latent_codes: bfloat16 [16, 12, 4, 256], P('tm', 'grp'), parts along dimension 1
- down_grad: float32 [4096, 256], P(('grp', 'tm')), parts along dimension 0
- coarse_grad: float32 [1536, 256], P(('grp', 'tm')), parts along dimension 0
- up_grad: float32 [512, 2048], P(('grp', 'tm')), parts along dimension 0
The draws below stay inside these ranges and needn't reach their ends.
There are 2 independent parts, one for each index of `grp`. The reference program is written for one: setup_inputs(seed, part) draws one part's arguments, and reference() takes and returns one part's arrays. A program takes and returns all parts, laid end to end along the dimension named above; an argument that names none is the same for every part. Nothing has to cross between parts.
All inputs are finite; a program needn't handle non-finite values.
Results may differ from the reference program's by a relative error of at most 0.018.
The reference program's roundings to bfloat16 on the way count: a program that leaves them out, or rounds other values in their place, can miss the bound.
Values may be sent and summed in bfloat16 or wider, within the bound.
A program may use at most 64 MiB of HBM per device.

```python
import math
import jax
import jax.numpy as jnp
from jax import lax

C = 256
H = 12
W = 8
T_SIZE = 32


def place_ends(drawn, key, least, largest):
    extent = drawn.shape
    spot = [jax.random.randint(jax.random.fold_in(key, axis), (), 0, extent[axis]) for axis in range(len(extent))]
    drawn = drawn.at[tuple(spot)].set(least)
    longest = extent.index(max(extent))
    spot[longest] = (spot[longest] + 1) % extent[longest]
    return drawn.at[tuple(spot)].set(largest)


def steps_of(stream_key, dims, cuts, low, high):
    factor_of, own = 1.0, jax.random.fold_in(stream_key, 6)
    for axis_at, blocks in cuts:
        draws = jnp.exp(jax.random.uniform(jax.random.fold_in(own, axis_at), (blocks,), jnp.float32, low / len(cuts), high / len(cuts)))
        factor_of = factor_of * jnp.repeat(draws, dims[axis_at] // blocks).reshape([-1 if axis == axis_at else 1 for axis in range(len(dims))])
    return factor_of


def noise(own_key, dims, width, limit, cuts=(), dtype=jnp.bfloat16):
    entries = width * jax.random.normal(own_key, dims, jnp.float32)
    if cuts:
        entries = entries * steps_of(own_key, dims, cuts, -0.22, 0.18)
    return jnp.clip(entries, -limit, limit).astype(dtype)


def setup_inputs(seed: int = 0, part: int = 0) -> dict:
    seeds = jax.random.split(jax.random.key(seed), 9)
    own_keys = jax.random.split(jax.random.fold_in(seeds[8], part), 9)
    video_features = noise(own_keys[0], (T_SIZE, H, W, C), 1.0, 6.0, ((0, 16),))
    cotangent = noise(own_keys[1], (T_SIZE, H, W, C), 1.0, 6.0, ((0, 16),))
    encoder_weight = noise(seeds[2], (27 * C, C), (27 * C) ** -0.5, 0.078125)
    down_weight = noise(seeds[3], (8 * C, C), (8 * C) ** -0.5, 0.125)
    coarse_weight = noise(seeds[4], (3 * C, C), (3 * C) ** -0.5, 0.21875)
    up_weight = noise(seeds[5], (C, 8 * C), C ** -0.5, 0.375)
    decoder_weight = noise(seeds[6], (27 * C, C), (27 * C) ** -0.5, 0.078125)
    levels = place_ends(jax.random.randint(seeds[7], (C,), 3, 9), jax.random.fold_in(seeds[7], 1), 3, 8).astype(jnp.int32)
    return {"video_features": video_features, "cotangent": cotangent, "encoder_weight": encoder_weight, "down_weight": down_weight, "coarse_weight": coarse_weight, "up_weight": up_weight, "decoder_weight": decoder_weight, "levels": levels}


two_pi = 2.0 * math.pi

def tap_rows(padded, frames, tile_rows, tile_cols):
    pieces = [padded[step_t:step_t + frames, step_r:step_r + tile_rows, step_c:step_c + tile_cols] for step_t in range(3) for step_r in range(3) for step_c in range(3)]
    return jnp.concatenate(pieces, axis=-1).reshape(frames * tile_rows * tile_cols, -1)

def flip_taps(weight, count):
    channels = weight.shape[1]
    blocks = weight.reshape(count, channels, channels)[::-1]
    return jnp.transpose(blocks, (0, 2, 1)).reshape(count * channels, channels)

def to_depth(field):
    frames, tile_rows, tile_cols, channels = field.shape
    split = field.reshape(frames // 2, 2, tile_rows // 2, 2, tile_cols // 2, 2, channels)
    return jnp.transpose(split, (0, 2, 4, 1, 3, 5, 6)).reshape(frames // 2, tile_rows // 2, tile_cols // 2, 8 * channels)

def from_depth(field):
    frames, tile_rows, tile_cols, packed = field.shape
    channels = packed // 8
    split = field.reshape(frames, tile_rows, tile_cols, 2, 2, 2, channels)
    return jnp.transpose(split, (0, 3, 1, 4, 2, 5, 6)).reshape(2 * frames, 2 * tile_rows, 2 * tile_cols, channels)

def transposed_product(left, right):
    return lax.dot_general(left, right, (((0,), (0,)), ((), ())), preferred_element_type=jnp.float32)

def product_with_transpose(left, right):
    return lax.dot_general(left, right, (((1,), (1,)), ((), ())), preferred_element_type=jnp.float32)

def time_columns(padded, frames):
    channels = padded.shape[-1]
    pieces = [padded[step_t:step_t + frames] for step_t in range(3)]
    return jnp.concatenate(pieces, axis=-1).reshape(-1, 3 * channels)

def reference(video_features, cotangent, encoder_weight, down_weight, coarse_weight, up_weight, decoder_weight, levels):
    frames, tile_rows, tile_cols, channels = video_features.shape
    fine_shape = video_features.shape
    grad_scale = 1.0 / math.sqrt(frames * tile_rows * tile_cols)
    half_range = (levels.astype(jnp.float32) - 1.0) * 0.5
    spatial = ((1, 1), (1, 1), (0, 0))
    past_pad = ((2, 0),) + spatial
    later_pad = ((0, 2),) + spatial
    enc_patches = tap_rows(jnp.pad(video_features, past_pad), frames, tile_rows, tile_cols)
    pre_enc = jnp.dot(enc_patches, encoder_weight, preferred_element_type=jnp.float32).reshape(fine_shape)
    hidden = (video_features.astype(jnp.float32) + jax.nn.silu(pre_enc)).astype(jnp.bfloat16)
    stacked = to_depth(hidden)
    coarse_shape = stacked.shape[:3] + (channels,)
    packed_shape = stacked.shape
    stacked_rows = stacked.reshape(-1, 8 * channels)
    latent = jnp.dot(stacked_rows, down_weight, preferred_element_type=jnp.float32).astype(jnp.bfloat16).reshape(coarse_shape)
    coarse_frames = coarse_shape[0]
    time_pad = ((2, 0), (0, 0), (0, 0), (0, 0))
    time_later = ((0, 2), (0, 0), (0, 0), (0, 0))
    latent_columns = time_columns(jnp.pad(latent, time_pad), coarse_frames)
    pre_code = jnp.dot(latent_columns, coarse_weight, preferred_element_type=jnp.float32)
    squashed = jnp.tanh(pre_code)
    bounded = half_range * squashed
    latent_codes = ((bounded - jnp.sin(two_pi * bounded) / two_pi) / half_range).astype(jnp.bfloat16)
    later_cot = tap_rows(jnp.pad(cotangent, later_pad), frames, tile_rows, tile_cols)
    back_dec = jnp.dot(later_cot, flip_taps(decoder_weight, 27), preferred_element_type=jnp.float32).reshape(fine_shape)
    decoded_grad = (cotangent.astype(jnp.float32) + back_dec).astype(jnp.bfloat16)
    depth_grad = to_depth(decoded_grad).reshape(-1, 8 * channels)
    code_grad = product_with_transpose(depth_grad, up_weight).astype(jnp.bfloat16)
    pre_grad = (code_grad.astype(jnp.float32) * (1.0 - jnp.cos(two_pi * bounded)) * (1.0 - squashed * squashed)).astype(jnp.bfloat16)
    later_columns = time_columns(jnp.pad(pre_grad.reshape(coarse_shape), time_later), coarse_frames)
    latent_grad = jnp.dot(later_columns, flip_taps(coarse_weight, 3), preferred_element_type=jnp.float32).astype(jnp.bfloat16)
    hidden_grad = from_depth(product_with_transpose(latent_grad, down_weight).reshape(packed_shape))
    sigmoid_pre = jax.nn.sigmoid(pre_enc)
    enc_pre_grad = (hidden_grad * sigmoid_pre * (1.0 + pre_enc * (1.0 - sigmoid_pre))).astype(jnp.bfloat16)
    later_enc = tap_rows(jnp.pad(enc_pre_grad, later_pad), frames, tile_rows, tile_cols)
    back_enc = jnp.dot(later_enc, flip_taps(encoder_weight, 27), preferred_element_type=jnp.float32).reshape(fine_shape)
    video_grad = (hidden_grad + back_enc).astype(jnp.bfloat16)
    down_grad = transposed_product(stacked_rows, latent_grad) * grad_scale
    coarse_grad = transposed_product(latent_columns, pre_grad) * grad_scale
    up_grad = transposed_product(latent_codes, depth_grad) * grad_scale
    return (video_grad, latent_codes.reshape(coarse_shape), down_grad, coarse_grad, up_grad)
```

```python
import functools
import math

import jax
import jax.numpy as jnp
import numpy as np
from jax import lax
from jax.experimental import pallas as pl
from jax.experimental.pallas import tpu as pltpu
from jax.sharding import PartitionSpec as P

two_pi = 2.0 * math.pi
BF = jnp.bfloat16
F32 = jnp.float32
MESH = pl.DeviceIdType.MESH

HALO_V, HALO_C, HALO_E = 0, 1, 2
LAT, PRE, COD, LGR, COLS, UPS = 0, 1, 2, 3, 4, 5


def mm(a, b):
    return jnp.dot(a, b, preferred_element_type=F32)


def mm_nt(a, b):
    return lax.dot_general(a, b, (((1,), (1,)), ((), ())), preferred_element_type=F32)


def mm_tn(a, b):
    return lax.dot_general(a, b, (((0,), (0,)), ((), ())), preferred_element_type=F32)


def depth_permutation(rows, cols):
    order = np.arange(2 * rows * cols).reshape(2, rows // 2, 2, cols // 2, 2)
    order = order.transpose(0, 2, 4, 1, 3).reshape(-1)
    picks = np.zeros((order.size, order.size), np.float32)
    picks[np.arange(order.size), order] = 1.0
    return picks


def kernel(
    n, scale, vf, ct, we, wd, wc, wu, wx, half, perm,
    vg_out, code_out, down_out, coarse_out, up_out,
    vbuf, cbuf, ebuf, we_v, wx_v, wd_v, wc_v, wu_v, perm_v, half_v,
    lat, pre, cod, lgr, cols_mine, cols_all, up_mine, up_all,
    vg_v, code_v, down_v, coarse_v, up_v, coarse_cut, up_cut,
    hal_s, hal_r, msg_s, msg_r, load_sem, out_sem,
):
    frames, rows, width, ch = vf.shape
    fine = frames * rows * width
    cells = fine // 8
    deep = wd.shape[0]
    nb, _, _, wb = cols_mine.shape
    rep = n // nb
    me = lax.axis_index("tm")

    def peer_of(k):
        return lax.rem(me + k, n)

    barrier = pltpu.get_barrier_semaphore()

    @pl.loop(1, n)
    def _(k):
        pl.semaphore_signal(barrier, inc=1, device_id={"tm": peer_of(k)}, device_id_type=MESH)

    third = we.shape[0] // 3
    loads = [
        pltpu.make_async_copy(vf, vbuf.at[2:4, 1 : rows + 1], load_sem.at[0]),
        pltpu.make_async_copy(ct, cbuf.at[0:2, 1 : rows + 1], load_sem.at[1]),
    ]
    for k, part in enumerate((2, 1, 0)):
        span = pl.ds(part * third, third)
        loads.append(pltpu.make_async_copy(we.at[span], we_v.at[span], load_sem.at[2 + k]))
        loads.append(pltpu.make_async_copy(wx.at[span], wx_v.at[span], load_sem.at[5 + k]))
    small = [
        pltpu.make_async_copy(src, dst, load_sem.at[8 + k])
        for k, (src, dst) in enumerate(
            ((perm, perm_v), (wd, wd_v), (wu, wu_v), (wc, wc_v), (half, half_v))
        )
    ]
    for load in loads[:4] + loads[4:] + small:
        load.start()

    def halo(kind, src, dst, peer):
        return pltpu.make_async_remote_copy(
            src_ref=src, dst_ref=dst, send_sem=hal_s.at[kind], recv_sem=hal_r.at[kind],
            device_id={"tm": peer}, device_id_type=MESH,
        )

    def message(kind, src, dst, peer, source):
        return pltpu.make_async_remote_copy(
            src_ref=src, dst_ref=dst, send_sem=msg_s.at[kind, peer], recv_sem=msg_r.at[kind, source],
            device_id={"tm": peer}, device_id_type=MESH,
        )

    first, last = me == 0, me == n - 1
    inner = pl.ds(1, rows)

    def rows_out(buf, at, out, cut, sem):
        count = out.shape[0]
        if count % 8 == 0:
            return pltpu.make_async_copy(buf.at[pl.ds(pl.multiple_of(at, 8), count)], out, sem)
        for k in range(count):
            cut[pl.ds(k, 1)] = buf[pl.ds(at + k, 1)]
        return pltpu.make_async_copy(cut, out, sem)

    def send_v():
        return halo(HALO_V, vf, vbuf.at[0:2, inner], me + 1)

    def send_c():
        return halo(HALO_C, ct, cbuf.at[2:4, inner], me - 1)

    def send_e():
        return halo(HALO_E, ebuf.at[0:2, inner], ebuf.at[2:4, inner], me - 1)

    edge = jnp.zeros((4, 1, width, ch), BF)
    for buf in (vbuf, cbuf, ebuf):
        buf[:, 0:1] = edge
        buf[:, rows + 1 : rows + 2] = edge
    blank = jnp.zeros((2, rows, width, ch), BF)

    @pl.when(first)
    def _():
        vbuf[0:2, 1 : rows + 1] = blank

    @pl.when(last)
    def _():
        cbuf[2:4, 1 : rows + 1] = blank
        ebuf[2:4, 1 : rows + 1] = blank

    lat[0:2] = jnp.zeros((2, cells, ch), BF)
    pre[n : n + 2] = jnp.zeros((2, cells, ch), BF)

    pl.semaphore_wait(barrier, n - 1)

    @pl.when(me < n - 1)
    def _():
        send_v().start()

    @pl.when(me > 0)
    def _():
        send_c().start()

    def taps(buf, p):
        return [buf[p : p + 2, q : q + rows].reshape(fine, ch) for q in range(3)]

    def past(buf, weight, p):
        left = jnp.concatenate(taps(buf, p), axis=1)
        out = []
        for r in range(3):
            right = jnp.concatenate(
                [weight[pl.ds(((3 * p + q) * 3 + r) * ch, ch)] for q in range(3)], axis=0
            )
            out.append(mm(left, right))
        return out

    def future(buf, weight, p):
        left = jnp.concatenate(taps(buf, p), axis=1)
        out = []
        for r in range(3):
            right = jnp.concatenate(
                [
                    weight[pl.ds((((2 - p) * 3 + 2 - q) * 3 + 2 - r) * ch, ch)]
                    for q in range(3)
                ],
                axis=1,
            )
            out.append(mm_nt(left, right))
        return out

    def added(a, b):
        return [x + y for x, y in zip(a, b)]

    lane = lax.broadcasted_iota(jnp.int32, (fine // width, width, ch), 1)

    def aligned(parts):
        a, b, c = [x.reshape(fine // width, width, ch) for x in parts]
        a = jnp.where(lane == 0, 0.0, pltpu.roll(a, 1, 1))
        c = jnp.where(lane == width - 1, 0.0, pltpu.roll(c, width - 1, 1))
        return (a + b + c).reshape(fine, ch)

    loads[0].wait()
    loads[2].wait()
    enc = past(vbuf, we_v, 2)
    loads[1].wait()
    loads[3].wait()
    dec = future(cbuf, wx_v, 0)
    loads[4].wait()
    loads[6].wait()

    @pl.when(me > 0)
    def _():
        send_v().wait_recv()

    enc = added(enc, past(vbuf, we_v, 1))
    enc = added(enc, past(vbuf, we_v, 0))
    pre_enc = aligned(enc)
    sig = jax.nn.sigmoid(pre_enc)
    own = vbuf[2:4, 1 : rows + 1].reshape(fine, ch).astype(F32)
    hidden = (own + pre_enc * sig).astype(BF)
    slope = sig * (1.0 + pre_enc * (1.0 - sig))

    for load in small:
        load.wait()

    def regroup(field):
        moved = mm(perm_v[0], field)
        return [moved[b * cells : (b + 1) * cells].astype(BF) for b in range(8)]

    def keep_columns(slot, blocks):
        per = nb // 8
        for b in range(8):
            for h in range(per):
                cols_mine[b * per + h, slot] = blocks[b][:, h * wb : (h + 1) * wb]

    stacked = regroup(hidden)
    keep_columns(0, stacked)
    lat[me + 2] = mm(jnp.concatenate(stacked, axis=1), wd_v[...]).astype(BF)

    def gather(buf, kind, slot, peer):
        return message(kind, buf.at[slot], buf.at[slot], peer, me)

    @pl.loop(1, n)
    def _(k):
        gather(lat, LAT, me + 2, peer_of(k)).start()

    loads[5].wait()
    loads[7].wait()

    @pl.when(me < n - 1)
    def _():
        send_c().wait_recv()

    dec = added(dec, future(cbuf, wx_v, 1))
    dec = added(dec, future(cbuf, wx_v, 2))
    own_c = cbuf[0:2, 1 : rows + 1].reshape(fine, ch).astype(F32)
    depth = regroup((own_c + aligned(dec)).astype(BF))
    keep_columns(1, depth)
    code_grad = mm_nt(jnp.concatenate(depth, axis=1), wu_v[...]).astype(BF)

    def columns(peer):
        return message(COLS, cols_mine.at[peer // rep], cols_all.at[me], peer, me)

    for lag in (1, 2):
        @pl.when(me >= lag)
        def _():
            message(LAT, lat.at[me + 2], lat.at[me + 2 - lag], me, me - lag).wait_recv()

    frames_in = jnp.concatenate([lat[me + p] for p in range(3)], axis=1)
    squashed = jnp.tanh(mm(frames_in, wc_v[...]))
    half_range = half_v[...]
    bounded = half_range * squashed
    codes = ((bounded - jnp.sin(two_pi * bounded) / two_pi) / half_range).astype(BF)
    factor = (1.0 - jnp.cos(two_pi * bounded)) * (1.0 - squashed * squashed)
    pre[me] = (code_grad.astype(F32) * factor).astype(BF)

    @pl.loop(1, n)
    def _(k):
        gather(pre, PRE, me, peer_of(n - k)).start()

    cod[me] = codes
    code_v[...] = codes.reshape(code_v.shape)
    code_copy = pltpu.make_async_copy(code_v, code_out, out_sem.at[0])
    code_copy.start()

    @pl.loop(1, n)
    def _(k):
        columns(peer_of(k)).start()

    cols_all[me] = cols_mine[me // rep]

    @pl.loop(1, n)
    def _(k):
        gather(cod, COD, me, peer_of(k)).start()

    for lag in (1, 2):
        @pl.when(me < n - lag)
        def _():
            message(PRE, pre.at[me], pre.at[me + lag], me, me + lag).wait_recv()

    wc_flip = jnp.concatenate([wc_v[pl.ds((2 - p) * ch, ch)] for p in range(3)], axis=1)
    later = jnp.concatenate([pre[me + p] for p in range(3)], axis=1)
    grad_lat = mm_nt(later, wc_flip).astype(BF)
    lgr[me] = grad_lat

    deep_grad = mm_nt(grad_lat, wd_v[...])
    deep_rows = jnp.concatenate(
        [deep_grad[:, b * ch : (b + 1) * ch] for b in range(8)], axis=0
    )
    high = deep_rows.astype(BF)
    rest = deep_rows - high.astype(F32)
    middle = rest.astype(BF)
    low = (rest - middle.astype(F32)).astype(BF)
    back = perm_v[1]
    hidden_grad = mm(back, high) + (mm(back, middle) + mm(back, low))
    ebuf[0:2, 1 : rows + 1] = (hidden_grad * slope).astype(BF).reshape(2, rows, width, ch)

    @pl.when(me > 0)
    def _():
        send_e().start()

    @pl.loop(1, n)
    def _(k):
        gather(lgr, LGR, me, peer_of(k)).start()

    bck = future(ebuf, we_v, 0)

    @pl.loop(1, n)
    def _(k):
        source = peer_of(n - k)

        @pl.when((k > 2) | (source > me))
        def _():
            message(LAT, lat.at[me + 2], lat.at[source + 2], me, source).wait_recv()

    @pl.loop(1, n)
    def _(k):
        source = peer_of(k)

        @pl.when((k > 2) | (source < me))
        def _():
            message(PRE, pre.at[me], pre.at[source], me, source).wait_recv()

    @pl.loop(1, n)
    def _(k):
        source = peer_of(k)
        message(COLS, cols_mine.at[0], cols_all.at[source], me, source).wait_recv()

    @pl.loop(1, n)
    def _(k):
        source = peer_of(k)
        message(COD, cod.at[me], cod.at[source], me, source).wait_recv()

    total = n * cells
    up_part = mm_tn(cod[...].reshape(total, ch), cols_all[:, 1].reshape(total, wb)) * scale
    blocks, block_rows = up_mine.shape[0], up_mine.shape[1]
    up_mine[...] = up_part.reshape(blocks, block_rows, wb)
    up_rows = ch // n
    mine = lax.rem(me, rep)
    my_block = me // rep

    def up_target(k):
        return mine + rep * lax.rem(my_block + k, nb)

    def up_send(peer):
        return message(
            UPS, up_mine.at[peer * up_rows // block_rows], up_all.at[my_block], peer, me
        )

    @pl.loop(1, nb)
    def _(k):
        up_send(up_target(k)).start()

    up_all[my_block] = up_mine[me * up_rows // block_rows]

    pre_all = pre[0:n].reshape(total, ch)
    for p in range(3):
        coarse_v[pl.ds(p * ch, ch)] = mm_tn(lat[p : p + n].reshape(total, ch), pre_all) * scale
    coarse_copy = rows_out(coarse_v, me * coarse_out.shape[0], coarse_out, coarse_cut, out_sem.at[1])
    coarse_copy.start()

    @pl.when(me < n - 1)
    def _():
        send_e().wait_recv()

    bck = added(bck, future(ebuf, we_v, 1))
    bck = added(bck, future(ebuf, we_v, 2))
    vg_v[...] = (hidden_grad + aligned(bck)).astype(BF).reshape(vg_v.shape)
    vg_copy = pltpu.make_async_copy(vg_v, vg_out, out_sem.at[2])
    vg_copy.start()

    @pl.loop(1, n)
    def _(k):
        source = peer_of(k)
        message(LGR, lgr.at[me], lgr.at[source], me, source).wait_recv()

    down_v[...] = (
        mm_tn(cols_all[:, 0].reshape(total, wb), lgr[...].reshape(total, ch)) * scale
    )
    down_rows = down_out.shape[0]
    down_copy = rows_out(down_v, mine * down_rows, down_out, None, out_sem.at[3])
    down_copy.start()

    @pl.loop(1, nb)
    def _(k):
        source = up_target(k)
        message(UPS, up_mine.at[0], up_all.at[source // rep], me, source).wait_recv()

    for b in range(nb):
        up_v[:, b * wb : (b + 1) * wb] = up_all[b]
    up_copy = rows_out(up_v, lax.rem(me * up_rows, block_rows), up_out, up_cut, out_sem.at[4])
    up_copy.start()

    @pl.when(me < n - 1)
    def _():
        send_v().wait_send()

    @pl.when(me > 0)
    def _():
        send_c().wait_send()
        send_e().wait_send()

    @pl.loop(1, n)
    def _(k):
        peer = peer_of(k)
        gather(lat, LAT, me + 2, peer).wait_send()
        gather(pre, PRE, me, peer).wait_send()
        gather(cod, COD, me, peer).wait_send()
        gather(lgr, LGR, me, peer).wait_send()
        columns(peer).wait_send()

    @pl.loop(1, nb)
    def _(k):
        up_send(up_target(k)).wait_send()

    for copy in (code_copy, coarse_copy, vg_copy, down_copy, up_copy):
        copy.wait()


def shards(n, vf, ct, we, wd, wc, wu, wx, levels):
    frames, rows, width, ch = vf.shape
    deep = wd.shape[0]
    fine = frames * rows * width
    cells = fine // 8
    wb = max(128, deep // n)
    nb = deep // wb
    up_rows = ch // n
    block_rows = max(8, up_rows)
    scale = 1.0 / math.sqrt(n * fine)
    half = ((levels.astype(F32) - 1.0) * 0.5).reshape(1, ch)
    picks = depth_permutation(rows, width)
    perm = jnp.asarray(np.stack([picks, picks.T]), BF)
    anywhere = pl.BlockSpec(memory_space=pl.ANY)
    code_shape = (frames // 2, rows // 2, width // 2, ch)
    out_shape = (
        jax.ShapeDtypeStruct(vf.shape, BF),
        jax.ShapeDtypeStruct(code_shape, BF),
        jax.ShapeDtypeStruct((deep // n, ch), F32),
        jax.ShapeDtypeStruct((wc.shape[0] // n, ch), F32),
        jax.ShapeDtypeStruct((up_rows, deep), F32),
    )
    padded = (4, rows + 2, width, ch)
    scratch = [
        pltpu.VMEM(padded, BF), pltpu.VMEM(padded, BF), pltpu.VMEM(padded, BF),
        pltpu.VMEM(we.shape, BF), pltpu.VMEM(wx.shape, BF), pltpu.VMEM(wd.shape, BF),
        pltpu.VMEM(wc.shape, BF), pltpu.VMEM(wu.shape, BF), pltpu.VMEM(perm.shape, BF),
        pltpu.VMEM(half.shape, F32),
        pltpu.VMEM((n + 2, cells, ch), BF), pltpu.VMEM((n + 2, cells, ch), BF),
        pltpu.VMEM((n, cells, ch), BF), pltpu.VMEM((n, cells, ch), BF),
        pltpu.VMEM((nb, 2, cells, wb), BF), pltpu.VMEM((n, 2, cells, wb), BF),
        pltpu.VMEM((ch // block_rows, block_rows, wb), F32),
        pltpu.VMEM((nb, block_rows, wb), F32),
        pltpu.VMEM(vf.shape, BF), pltpu.VMEM(code_shape, BF), pltpu.VMEM((wb, ch), F32),
        pltpu.VMEM(wc.shape, F32), pltpu.VMEM((block_rows, deep), F32),
        pltpu.VMEM(out_shape[3].shape, F32), pltpu.VMEM(out_shape[4].shape, F32),
        pltpu.SemaphoreType.DMA((3,)), pltpu.SemaphoreType.DMA((3,)),
        pltpu.SemaphoreType.DMA((6, n)), pltpu.SemaphoreType.DMA((6, n)),
        pltpu.SemaphoreType.DMA((13,)), pltpu.SemaphoreType.DMA((5,)),
    ]
    return pl.pallas_call(
        functools.partial(kernel, n, scale),
        out_shape=out_shape,
        in_specs=[anywhere] * 9,
        out_specs=(anywhere,) * 5,
        scratch_shapes=scratch,
        compiler_params=pltpu.CompilerParams(collective_id=0, has_side_effects=True),
    )(vf, ct, we, wd, wc, wu, wx, half, perm)


def solution(mesh):
    placed = (P("tm", "grp", None, None), P("tm", "grp", None, None), P(), P(), P(), P(), P(), P())
    return jax.shard_map(
        functools.partial(shards, mesh.shape["tm"]),
        mesh=mesh,
        in_specs=placed,
        out_specs=(
            P("tm", "grp", None, None),
            P("tm", "grp", None, None),
            P(("grp", "tm"), None),
            P(("grp", "tm"), None),
            P(("grp", "tm"), None),
        ),
        check_vma=False,
    )
```

```python
import functools
import math

import jax
import jax.numpy as jnp
import numpy as np
from jax import lax
from jax.experimental import pallas as pl
from jax.experimental.pallas import tpu as pltpu
from jax.sharding import PartitionSpec as P

two_pi = 2.0 * math.pi
BF = jnp.bfloat16
F32 = jnp.float32
MESH = pl.DeviceIdType.MESH

HALO_V, HALO_C, HALO_N = 0, 1, 2
LAT, CGR, STK, DEP, UPS = 0, 1, 2, 3, 4

NEAR = (1, 2, -1, -2, -3)


def mm(a, b):
    return jnp.dot(a, b, preferred_element_type=F32)


def mm_nt(a, b):
    return lax.dot_general(a, b, (((1,), (1,)), ((), ())), preferred_element_type=F32)


def mm_tn(a, b):
    return lax.dot_general(a, b, (((0,), (0,)), ((), ())), preferred_element_type=F32)


def depth_permutation(rows, cols):
    order = np.arange(2 * rows * cols).reshape(2, rows // 2, 2, cols // 2, 2)
    order = order.transpose(0, 2, 4, 1, 3).reshape(-1)
    picks = np.zeros((order.size, order.size), np.float32)
    picks[np.arange(order.size), order] = 1.0
    return picks


def kernel(
    n, scale, vf, ct, we, wd, wc, wu, wx, levels, perm,
    vg_out, code_out, down_out, coarse_out, up_out,
    vbuf, cbuf, ebuf, we_v, wx_v, wd_v, wc_v, wu_v, perm_v, level_v,
    lat, cgr, cod, fac, pre, lgr, stk_mine, stk_all, dep_mine, dep_all, up_mine, up_all, coarse_v, whole_v,
    hal_s, hal_r, msg_s, msg_r, fwd_s, load_sem,
):
    frames, rows, width, ch = vf.shape
    fine = frames * rows * width
    cells = fine // 8
    nb, _, wb = stk_mine.shape
    rep = n // nb
    me = lax.axis_index("tm")

    def peer_of(k):
        return lax.rem(me + k, n)

    barrier = pltpu.get_barrier_semaphore()

    @pl.loop(1, n)
    def _(k):
        pl.semaphore_signal(barrier, inc=1, device_id={"tm": peer_of(k)}, device_id_type=MESH)

    inner = pl.ds(1, rows)
    third = we.shape[0] // 3
    loads = [
        pltpu.make_async_copy(vf, vbuf.at[2:4, inner], load_sem.at[0]),
        pltpu.make_async_copy(ct, cbuf.at[0:2, inner], load_sem.at[1]),
    ]
    for k, part in enumerate((2, 1, 0)):
        span = pl.ds(part * third, third)
        loads.append(pltpu.make_async_copy(we.at[span], we_v.at[span], load_sem.at[2 + 2 * k]))
        loads.append(pltpu.make_async_copy(wx.at[span], wx_v.at[span], load_sem.at[3 + 2 * k]))
    small = [
        pltpu.make_async_copy(src, dst, load_sem.at[8 + k])
        for k, (src, dst) in enumerate(
            ((perm, perm_v), (wd, wd_v), (wu, wu_v), (wc, wc_v), (levels, level_v))
        )
    ]
    for load in loads + small:
        load.start()

    def halo(kind, src, dst, peer):
        return pltpu.make_async_remote_copy(
            src_ref=src, dst_ref=dst, send_sem=hal_s.at[kind], recv_sem=hal_r.at[kind],
            device_id={"tm": peer}, device_id_type=MESH,
        )

    def message(kind, src, dst, peer, source, sends=None):
        return pltpu.make_async_remote_copy(
            src_ref=src, dst_ref=dst,
            send_sem=msg_s.at[kind, peer] if sends is None else sends,
            recv_sem=msg_r.at[kind, source],
            device_id={"tm": peer}, device_id_type=MESH,
        )

    def send_v():
        return halo(HALO_V, vf, vbuf.at[0:2, inner], me + 1)

    def send_c():
        return halo(HALO_C, ct, cbuf.at[2:4, inner], me - 1)

    def send_n():
        return halo(HALO_N, vf, vbuf.at[4:6, inner], me - 1)

    for buf in (vbuf, cbuf, ebuf):
        edge = jnp.zeros((buf.shape[0], 1, width, ch), BF)
        buf[:, 0:1] = edge
        buf[:, rows + 1 : rows + 2] = edge
    blank = jnp.zeros((2, rows, width, ch), BF)

    @pl.when(me == 0)
    def _():
        vbuf[0:2, 1 : rows + 1] = blank

    @pl.when(me == n - 1)
    def _():
        cbuf[2:4, 1 : rows + 1] = blank
        vbuf[4:6, 1 : rows + 1] = blank

    lat[0:2] = jnp.zeros((2, cells, ch), BF)
    lat[n + 2 : n + 5] = jnp.zeros((3, cells, ch), BF)
    cgr[n : n + 3] = jnp.zeros((3, cells, ch), BF)
    pre[n : n + 2] = jnp.zeros((2, cells, ch), BF)

    pl.semaphore_wait(barrier, n - 1)

    @pl.when(me < n - 1)
    def _():
        send_v().start()

    @pl.when(me > 0)
    def _():
        send_c().start()
        send_n().start()

    def taps(buf, at):
        return jnp.concatenate(
            [buf[at : at + 2, q : q + rows].reshape(fine, ch) for q in range(3)], axis=1
        )

    def past(buf, at, weight, p):
        left = taps(buf, at + p)
        out = []
        for r in range(3):
            right = jnp.concatenate(
                [weight[pl.ds(((3 * p + q) * 3 + r) * ch, ch)] for q in range(3)], axis=0
            )
            out.append(mm(left, right))
        return out

    def future(buf, at, weight, p):
        left = taps(buf, at + p)
        out = []
        for r in range(3):
            right = jnp.concatenate(
                [
                    weight[pl.ds((((2 - p) * 3 + 2 - q) * 3 + 2 - r) * ch, ch)]
                    for q in range(3)
                ],
                axis=1,
            )
            out.append(mm_nt(left, right))
        return out

    def added(a, b):
        return [x + y for x, y in zip(a, b)]

    lane = lax.broadcasted_iota(jnp.int32, (fine // width, width, ch), 1)

    def aligned(parts):
        a, b, c = [x.reshape(fine // width, width, ch) for x in parts]
        a = jnp.where(lane == 0, 0.0, pltpu.roll(a, 1, 1))
        c = jnp.where(lane == width - 1, 0.0, pltpu.roll(c, width - 1, 1))
        return (a + b + c).reshape(fine, ch)

    loads[0].wait()
    loads[2].wait()
    enc = past(vbuf, 0, we_v, 2)
    loads[1].wait()
    loads[7].wait()
    loads[3].wait()
    dec = future(cbuf, 0, wx_v, 0)
    loads[4].wait()
    loads[6].wait()

    @pl.when(me > 0)
    def _():
        send_v().wait_recv()

    enc = added(enc, past(vbuf, 0, we_v, 1))
    enc = added(enc, past(vbuf, 0, we_v, 0))
    pre_enc = aligned(enc)
    sig = jax.nn.sigmoid(pre_enc)
    own = vbuf[2:4, 1 : rows + 1].reshape(fine, ch).astype(F32)
    hidden = (own + pre_enc * sig).astype(BF)

    def slope_of(x, s):
        return s * (1.0 + x * (1.0 - s))

    slope = slope_of(pre_enc, sig)

    for load in small:
        load.wait()

    def regroup(field, store):
        moved = mm(perm_v[0], field)
        blocks = [moved[b * cells : (b + 1) * cells].astype(BF) for b in range(8)]
        per = nb // 8
        for b in range(8):
            for h in range(per):
                store[b * per + h] = blocks[b][:, h * wb : (h + 1) * wb]
        return jnp.concatenate(blocks, axis=1)

    buddy = me + 1 - 2 * lax.rem(me, 2)

    def slot_send(buf, kind, slot, peer):
        return message(kind, buf.at[slot], buf.at[slot], peer, me)

    def inside(k):
        return (me + k >= 0) & (me + k < n)

    def spread(buf, kind, slot, act):
        for k in NEAR:
            @pl.when(inside(k))
            def _():
                act(slot_send(buf, kind, slot, me + k))

        @pl.loop(1, n // 2)
        def _(k):
            peer = lax.rem(me + 2 * k, n)
            @pl.when(((peer - me) != 2) & ((peer - me) != -2))
            def _():
                act(slot_send(buf, kind, slot, peer))

    def near_odd(diff):
        return (diff == 1) | (diff == -1) | (diff == -3)

    def arrival(buf, kind, shift, source):
        return message(kind, buf.at[me + shift], buf.at[source + shift], me, source)

    def forward(buf, kind, shift, source):
        slot = source + shift
        return message(kind, buf.at[slot], buf.at[slot], buddy, source, fwd_s.at[kind, source])

    def relay(buf, kind, shift, near):
        @pl.loop(1, n // 2)
        def _(k):
            source = lax.rem(me + n - 2 * k, n)
            diff = source - me
            done = functools.reduce(jnp.logical_or, [diff == d for d in near])

            @pl.when(jnp.logical_not(done))
            def _():
                arrival(buf, kind, shift, source).wait_recv()

            @pl.when(jnp.logical_not(near_odd(buddy - source)))
            def _():
                forward(buf, kind, shift, source).start()

    def collect(buf, kind, shift, near):
        @pl.loop(0, n // 2)
        def _(k):
            source = lax.rem(buddy + 2 * k, n)
            diff = source - me
            done = functools.reduce(jnp.logical_or, [diff == d for d in near])

            @pl.when(jnp.logical_not(done))
            def _():
                arrival(buf, kind, shift, source).wait_recv()

    def start(copy):
        copy.start()

    def wait_send(copy):
        copy.wait_send()

    lat[me + 2] = mm(regroup(hidden, stk_mine), wd_v[...]).astype(BF)
    spread(lat, LAT, me + 2, start)

    loads[5].wait()

    @pl.when(me < n - 1)
    def _():
        send_c().wait_recv()

    dec = added(dec, future(cbuf, 0, wx_v, 1))
    dec = added(dec, future(cbuf, 0, wx_v, 2))
    own_c = cbuf[0:2, 1 : rows + 1].reshape(fine, ch).astype(F32)
    depth = regroup((own_c + aligned(dec)).astype(BF), dep_mine)
    cgr[me] = mm_nt(depth, wu_v[...]).astype(BF)
    spread(cgr, CGR, me, start)

    def block_send(kind, mine, everyone, peer):
        return message(kind, mine.at[peer // rep], everyone.at[me], peer, me)

    @pl.loop(1, n)
    def _(k):
        block_send(DEP, dep_mine, dep_all, peer_of(k)).start()

    @pl.loop(1, n)
    def _(k):
        block_send(STK, stk_mine, stk_all, peer_of(k)).start()

    dep_all[me] = dep_mine[me // rep]
    stk_all[me] = stk_mine[me // rep]

    @pl.when(me < n - 1)
    def _():
        send_n().wait_recv()

    ahead = past(vbuf, 2, we_v, 0)
    ahead = added(ahead, past(vbuf, 2, we_v, 1))
    ahead = aligned(added(ahead, past(vbuf, 2, we_v, 2)))
    slope_next = slope_of(ahead, jax.nn.sigmoid(ahead))

    half = ((level_v[...].astype(F32) - 1.0) * 0.5).reshape(1, ch)

    def coder(frame, count):
        columns = jnp.concatenate(
            [lat[pl.ds(frame + p, count)].reshape(count * cells, ch) for p in range(3)], axis=1
        )
        squashed = jnp.tanh(mm(columns, wc_v[...]))
        bounded = half * squashed
        codes = ((bounded - jnp.sin(two_pi * bounded) / two_pi) / half).astype(BF)
        return codes, (1.0 - jnp.cos(two_pi * bounded)) * (1.0 - squashed * squashed)

    wc_flip = jnp.concatenate([wc_v[pl.ds((2 - p) * ch, ch)] for p in range(3)], axis=1)

    lat_near = (-1, -2, 1, 2, 3)
    cgr_near = (1, 2, 3)
    for k in lat_near:
        @pl.when(inside(k))
        def _():
            arrival(lat, LAT, 2, me + k).wait_recv()

    codes, factor = coder(me, 4)
    code_out[...] = codes[0:cells].reshape(code_out.shape)
    for k in cgr_near:
        @pl.when(inside(k))
        def _():
            arrival(cgr, CGR, 0, me + k).wait_recv()

    ahead_grad = cgr[pl.ds(me, 4)].reshape(4 * cells, ch).astype(F32) * factor
    later = jnp.concatenate(
        [ahead_grad[p * cells : (p + 2) * cells].astype(BF) for p in range(3)], axis=1
    )
    grad_lat = mm_nt(later, wc_flip).astype(BF)

    deep_grad = mm_nt(grad_lat, wd_v[...])
    back = perm_v[1]
    hidden_grads = []
    for frame in range(2):
        deep_rows = jnp.concatenate(
            [
                deep_grad[frame * cells : (frame + 1) * cells, b * ch : (b + 1) * ch]
                for b in range(8)
            ],
            axis=0,
        )
        high = deep_rows.astype(BF)
        rest = deep_rows - high.astype(F32)
        middle = rest.astype(BF)
        low = (rest - middle.astype(F32)).astype(BF)
        hidden_grads.append(mm(back, high) + (mm(back, middle) + mm(back, low)))
    for frame, weight in enumerate((slope, slope_next)):
        ebuf[2 * frame : 2 * frame + 2, 1 : rows + 1] = (
            (hidden_grads[frame] * weight).astype(BF).reshape(2, rows, width, ch)
        )

    relay(lat, LAT, 2, lat_near)
    bck = future(ebuf, 0, we_v, 0)
    bck = added(bck, future(ebuf, 0, we_v, 1))
    bck = added(bck, future(ebuf, 0, we_v, 2))
    vg_out[...] = (hidden_grads[0] + aligned(bck)).astype(BF).reshape(vg_out.shape)
    relay(cgr, CGR, 0, cgr_near)

    collect(lat, LAT, 2, lat_near)
    step = 4
    total = n * cells

    @pl.loop(0, n // step)
    def _(k):
        at = k * step
        codes, factor = coder(at, step)
        cod[pl.ds(at, step)] = codes.reshape(step, cells, ch)
        fac[pl.ds(at, step)] = factor.reshape(step, cells, ch)

    @pl.loop(1, n)
    def _(k):
        source = peer_of(k)
        message(DEP, dep_mine.at[0], dep_all.at[source], me, source).wait_recv()

    up_part = mm_tn(cod[...].reshape(total, ch), dep_all[...].reshape(total, wb)) * scale
    block_rows = up_mine.shape[1]
    up_mine[...] = up_part.reshape(up_mine.shape)
    up_rows = ch // n
    mine = lax.rem(me, rep)
    my_block = me // rep

    def up_target(k):
        return mine + rep * lax.rem(my_block + k, nb)

    def up_send(peer):
        return message(
            UPS, up_mine.at[peer * up_rows // block_rows], up_all.at[my_block], peer, me
        )

    @pl.loop(1, nb)
    def _(k):
        up_send(up_target(k)).start()

    up_all[my_block] = up_mine[me * up_rows // block_rows]

    def take_rows(buf, at, out):
        count = out.shape[0]
        if count % 8 == 0:
            out[...] = buf[pl.ds(pl.multiple_of(at, 8), count)]
        else:
            for k in range(count):
                out[pl.ds(k, 1)] = buf[pl.ds(at + k, 1)]

    collect(cgr, CGR, 0, cgr_near)
    pre[0:n] = (cgr[0:n].astype(F32) * fac[...]).astype(BF)
    pre_all = pre[0:n].reshape(total, ch)
    for p in range(3):
        coarse_v[pl.ds(p * ch, ch)] = mm_tn(lat[p : p + n].reshape(total, ch), pre_all) * scale
    take_rows(coarse_v, me * coarse_out.shape[0], coarse_out)
    later_all = jnp.concatenate([pre[p : p + n].reshape(total, ch) for p in range(3)], axis=1)
    lgr[...] = mm_nt(later_all, wc_flip).astype(BF).reshape(lgr.shape)

    @pl.loop(1, n)
    def _(k):
        source = peer_of(k)
        message(STK, stk_mine.at[0], stk_all.at[source], me, source).wait_recv()

    whole_v[0:wb, 0:ch] = (
        mm_tn(stk_all[...].reshape(total, wb), lgr[...].reshape(total, ch)) * scale
    )
    take_rows(whole_v.at[:, pl.ds(0, ch)], mine * down_out.shape[0], down_out)

    @pl.loop(1, nb)
    def _(k):
        source = up_target(k)
        message(UPS, up_mine.at[0], up_all.at[source // rep], me, source).wait_recv()

    up_at = lax.rem(me * up_rows, block_rows)
    for b in range(nb):
        take_rows(up_all.at[b], up_at, up_out.at[:, pl.ds(b * wb, wb)])

    @pl.when(me < n - 1)
    def _():
        send_v().wait_send()

    @pl.when(me > 0)
    def _():
        send_c().wait_send()
        send_n().wait_send()

    for buf, kind, shift in ((lat, LAT, 2), (cgr, CGR, 0)):
        spread(buf, kind, me + shift, wait_send)

        @pl.loop(1, n // 2)
        def _(k):
            source = lax.rem(me + n - 2 * k, n)

            @pl.when(jnp.logical_not(near_odd(buddy - source)))
            def _():
                forward(buf, kind, shift, source).wait_send()

    @pl.loop(1, n)
    def _(k):
        block_send(DEP, dep_mine, dep_all, peer_of(k)).wait_send()
        block_send(STK, stk_mine, stk_all, peer_of(k)).wait_send()

    @pl.loop(1, nb)
    def _(k):
        up_send(up_target(k)).wait_send()


def tail(*refs):
    sems = refs[-1]
    count = len(refs) // 2
    copies = [pltpu.make_async_copy(refs[k], refs[count + k], sems.at[k]) for k in range(count)]
    for copy in copies:
        copy.start()
    for copy in copies:
        copy.wait()


def shards(n, vf, ct, we, wd, wc, wu, wx, levels):
    frames, rows, width, ch = vf.shape
    deep = wd.shape[0]
    fine = frames * rows * width
    cells = fine // 8
    wb = max(128, deep // n)
    nb = deep // wb
    up_rows = ch // n
    block_rows = max(8, up_rows)
    scale = 1.0 / math.sqrt(n * fine)
    picks = depth_permutation(rows, width)
    perm = jnp.asarray(np.stack([picks, picks.T]), BF)
    anywhere = pl.BlockSpec(memory_space=pl.ANY)
    results = (
        (vf.shape, BF),
        ((frames // 2, rows // 2, width // 2, ch), BF),
        ((deep // n, ch), F32),
        ((wc.shape[0] // n, ch), F32),
        ((up_rows, deep), F32),
    )
    four = (4, rows + 2, width, ch)
    scratch = [
        pltpu.VMEM((6, rows + 2, width, ch), BF), pltpu.VMEM(four, BF), pltpu.VMEM(four, BF),
        pltpu.VMEM(we.shape, BF), pltpu.VMEM(wx.shape, BF), pltpu.VMEM(wd.shape, BF),
        pltpu.VMEM(wc.shape, BF), pltpu.VMEM(wu.shape, BF), pltpu.VMEM(perm.shape, BF),
        pltpu.VMEM(levels.shape, jnp.int32),
        pltpu.VMEM((n + 5, cells, ch), BF), pltpu.VMEM((n + 3, cells, ch), BF),
        pltpu.VMEM((n, cells, ch), BF), pltpu.VMEM((n, cells, ch), F32),
        pltpu.VMEM((n + 2, cells, ch), BF), pltpu.VMEM((n, cells, ch), BF),
        pltpu.VMEM((nb, cells, wb), BF), pltpu.VMEM((n, cells, wb), BF),
        pltpu.VMEM((nb, cells, wb), BF), pltpu.VMEM((n, cells, wb), BF),
        pltpu.VMEM((ch // block_rows, block_rows, wb), F32),
        pltpu.VMEM((nb, block_rows, wb), F32),
        pltpu.VMEM(wc.shape, F32), pltpu.VMEM((wb, ch), F32),
        pltpu.SemaphoreType.DMA((3,)), pltpu.SemaphoreType.DMA((3,)),
        pltpu.SemaphoreType.DMA((5, n)), pltpu.SemaphoreType.DMA((5, n)),
        pltpu.SemaphoreType.DMA((2, n)), pltpu.SemaphoreType.DMA((13,)),
    ]
    held = pl.pallas_call(
        functools.partial(kernel, n, scale),
        out_shape=tuple(pltpu.VMEM(*result) for result in results),
        in_specs=[anywhere] * 9,
        out_specs=(pl.BlockSpec(memory_space=pltpu.VMEM),) * 5,
        scratch_shapes=scratch,
        compiler_params=pltpu.CompilerParams(collective_id=0, has_side_effects=True),
    )(vf, ct, we, wd, wc, wu, wx, levels, perm)
    return pl.pallas_call(
        tail,
        out_shape=tuple(jax.ShapeDtypeStruct(*result) for result in results),
        in_specs=[anywhere] * 5,
        out_specs=(anywhere,) * 5,
        scratch_shapes=[pltpu.SemaphoreType.DMA((5,))],
    )(*[pltpu.with_memory_space_constraint(part, pltpu.VMEM) for part in held])


def solution(mesh):
    placed = (P("tm", "grp", None, None), P("tm", "grp", None, None), P(), P(), P(), P(), P(), P())
    return jax.shard_map(
        functools.partial(shards, mesh.shape["tm"]),
        mesh=mesh,
        in_specs=placed,
        out_specs=(
            P("tm", "grp", None, None),
            P("tm", "grp", None, None),
            P(("grp", "tm"), None),
            P(("grp", "tm"), None),
            P(("grp", "tm"), None),
        ),
        check_vma=False,
    )
```

```python
import functools
import math

import jax
import jax.numpy as jnp
import numpy as np
from jax import lax
from jax.experimental import pallas as pl
from jax.experimental.pallas import tpu as pltpu
from jax.sharding import PartitionSpec as P

two_pi = 2.0 * math.pi
BF = jnp.bfloat16
F32 = jnp.float32
MESH = pl.DeviceIdType.MESH

HALO_V, HALO_C, HALO_N = 0, 1, 2
LAT, CGR = 0, 1
STK, DEP, UPS = 0, 1, 2

SINE = [(-1.0) ** k / math.factorial(2 * k + 1) for k in range(7)]
COSINE = [(-1.0) ** k / math.factorial(2 * k) for k in range(7)]

NEAR = (1, 2, -1, -2, -3)


def mm(a, b):
    return jnp.dot(a, b, preferred_element_type=F32)


def mm_nt(a, b):
    return lax.dot_general(a, b, (((1,), (1,)), ((), ())), preferred_element_type=F32)


def mm_tn(a, b):
    return lax.dot_general(a, b, (((0,), (0,)), ((), ())), preferred_element_type=F32)


def half_turn(x):
    angle = (x - jnp.round(x)) * math.pi
    square = angle * angle
    sine, cosine = SINE[-1], COSINE[-1]
    for a, b in zip(SINE[-2::-1], COSINE[-2::-1]):
        sine = sine * square + a
        cosine = cosine * square + b
    return sine * angle, cosine


def depth_permutation(rows, cols):
    order = np.arange(2 * rows * cols).reshape(2, rows // 2, 2, cols // 2, 2)
    order = order.transpose(0, 2, 4, 1, 3).reshape(-1)
    picks = np.zeros((order.size, order.size), np.float32)
    picks[np.arange(order.size), order] = 1.0
    return picks


def kernel(
    n, scale, vf, ct, we, wd, wc, wu, wx, levels, perm,
    vg_out, code_out, down_out, coarse_out, up_out,
    vbuf, cbuf, ebuf, we_v, wx_v, wd_v, wc_v, wu_v, perm_v, level_v,
    lat, cgr, cod, fac, pre, lgr, stk_mine, stk_all, dep_mine, dep_all, up_mine, up_all, coarse_v, whole_v,
    acc_e, acc_d, hal_s, hal_r, msg_s, msg_r, fwd_s, all_s, all_r, load_sem, met,
):
    frames, rows, width, ch = vf.shape
    fine = frames * rows * width
    cells = fine // 8
    nb, _, wb = stk_mine.shape
    rep = n // nb
    me = lax.axis_index("tm")

    def peer_of(k):
        return lax.rem(me + k, n)

    odd = lax.rem(me, 2)
    buddy = me + 1 - 2 * odd
    other = me - 1 + 2 * odd
    has_other = (other >= 0) & (other < n)
    dims = n.bit_length() - 1

    def partner(d):
        return me + (1 - 2 * lax.rem(me // 2**d, 2)) * 2**d

    barrier = pltpu.get_barrier_semaphore()
    for d in range(dims):
        pl.semaphore_signal(barrier, inc=1, device_id={"tm": partner(d)}, device_id_type=MESH)

    @pl.when(has_other)
    def _():
        pl.semaphore_signal(barrier, inc=1, device_id={"tm": other}, device_id_type=MESH)

    def tell(d):
        if d < dims:
            pl.semaphore_signal(
                met.at[d], inc=1, device_id={"tm": partner(d)}, device_id_type=MESH
            )

    def hear(d):
        if d < dims:
            pl.semaphore_wait(met.at[d], 1)

    inner = pl.ds(1, rows)
    third = we.shape[0] // 3
    loads = [
        pltpu.make_async_copy(vf, vbuf.at[2:4, inner], load_sem.at[0]),
        pltpu.make_async_copy(ct, cbuf.at[0:2, inner], load_sem.at[1]),
    ]
    for k, part in enumerate((2, 1, 0)):
        span = pl.ds(part * third, third)
        loads.append(pltpu.make_async_copy(we.at[span], we_v.at[span], load_sem.at[2 + 2 * k]))
        loads.append(pltpu.make_async_copy(wx.at[span], wx_v.at[span], load_sem.at[3 + 2 * k]))
    small = [
        pltpu.make_async_copy(src, dst, load_sem.at[8 + k])
        for k, (src, dst) in enumerate(
            ((perm, perm_v), (wd, wd_v), (wu, wu_v), (wc, wc_v), (levels, level_v))
        )
    ]
    for load in loads + small:
        load.start()

    def halo(kind, src, dst, peer):
        return pltpu.make_async_remote_copy(
            src_ref=src, dst_ref=dst, send_sem=hal_s.at[kind], recv_sem=hal_r.at[kind],
            device_id={"tm": peer}, device_id_type=MESH,
        )

    def message(kind, src, dst, peer, source, sends=None):
        return pltpu.make_async_remote_copy(
            src_ref=src, dst_ref=dst,
            send_sem=msg_s.at[kind, peer] if sends is None else sends,
            recv_sem=msg_r.at[kind, source],
            device_id={"tm": peer}, device_id_type=MESH,
        )

    def block(kind, src, dst, peer):
        return pltpu.make_async_remote_copy(
            src_ref=src, dst_ref=dst, send_sem=all_s.at[kind], recv_sem=all_r.at[kind],
            device_id={"tm": peer}, device_id_type=MESH,
        )

    def all_blocks(kind, buf, count):
        return block(kind, buf.at[pl.ds(0, count)], buf.at[pl.ds(0, count)], buddy)

    def send_v():
        return halo(HALO_V, vf, vbuf.at[0:2, inner], me + 1)

    def send_c():
        return halo(HALO_C, ct, cbuf.at[2:4, inner], me - 1)

    def send_n():
        return halo(HALO_N, vf, vbuf.at[4:6, inner], me - 1)

    for buf in (vbuf, cbuf, ebuf):
        edge = jnp.zeros((buf.shape[0], 1, width, ch), BF)
        buf[:, 0:1] = edge
        buf[:, rows + 1 : rows + 2] = edge
    blank = jnp.zeros((2, rows, width, ch), BF)

    @pl.when(me == 0)
    def _():
        vbuf[0:2, 1 : rows + 1] = blank

    @pl.when(me == n - 1)
    def _():
        cbuf[2:4, 1 : rows + 1] = blank
        vbuf[4:6, 1 : rows + 1] = blank

    lat[0:2] = jnp.zeros((2, cells, ch), BF)
    lat[n + 2 : n + 5] = jnp.zeros((3, cells, ch), BF)
    cgr[n : n + 3] = jnp.zeros((3, cells, ch), BF)
    pre[0:2] = jnp.zeros((2, cells, ch), BF)
    pre[n + 2 : n + 4] = jnp.zeros((2, cells, ch), BF)

    pl.semaphore_wait(barrier, jnp.where(has_other, dims + 1, dims))
    tell(0)

    @pl.when(me < n - 1)
    def _():
        send_v().start()

    @pl.when(me > 0)
    def _():
        send_c().start()
        send_n().start()

    def taps(buf, at):
        return jnp.concatenate(
            [buf[at : at + 2, q : q + rows].reshape(fine, ch) for q in range(3)], axis=1
        )

    def past(buf, at, weight, parts):
        left = jnp.concatenate([taps(buf, at + p) for p in parts], axis=1)
        out = []
        for r in range(3):
            right = jnp.concatenate(
                [
                    weight[pl.ds(((3 * p + q) * 3 + r) * ch, ch)]
                    for p in parts
                    for q in range(3)
                ],
                axis=0,
            )
            out.append(mm(left, right))
        return out

    def future(buf, at, weight, parts):
        left = jnp.concatenate([taps(buf, at + p) for p in parts], axis=1)
        out = []
        for r in range(3):
            right = jnp.concatenate(
                [
                    weight[pl.ds((((2 - p) * 3 + 2 - q) * 3 + 2 - r) * ch, ch)]
                    for p in parts
                    for q in range(3)
                ],
                axis=1,
            )
            out.append(mm_nt(left, right))
        return out

    def keep(acc, parts):
        for r in range(3):
            acc[r] = parts[r]

    def added(acc, parts):
        return [acc[r] + parts[r] for r in range(3)]

    lane = lax.broadcasted_iota(jnp.int32, (fine // width, width, ch), 1)

    def aligned(parts):
        a, b, c = [x.reshape(fine // width, width, ch) for x in parts]
        a = jnp.where(lane == 0, 0.0, pltpu.roll(a, 1, 1))
        c = jnp.where(lane == width - 1, 0.0, pltpu.roll(c, width - 1, 1))
        return (a + b + c).reshape(fine, ch)

    loads[0].wait()
    loads[2].wait()
    keep(acc_e, past(vbuf, 0, we_v, (2,)))
    hear(0)
    tell(1)
    loads[1].wait()
    loads[3].wait()
    keep(acc_d, future(cbuf, 0, wx_v, (0,)))
    hear(1)
    tell(2)
    loads[4].wait()
    loads[6].wait()

    @pl.when(me > 0)
    def _():
        send_v().wait_recv()

    hear(2)
    tell(3)
    enc = added(acc_e, past(vbuf, 0, we_v, (1, 0)))
    pre_enc = aligned(enc)
    sig = jax.nn.sigmoid(pre_enc)
    own = vbuf[2:4, 1 : rows + 1].reshape(fine, ch).astype(F32)
    hidden = (own + pre_enc * sig).astype(BF)

    def slope_of(x, s):
        return s * (1.0 + x * (1.0 - s))

    for load in small:
        load.wait()

    def regroup(field, store):
        moved = mm(perm_v[0], field)
        blocks = [moved[b * cells : (b + 1) * cells].astype(BF) for b in range(8)]
        per = nb // 8
        for b in range(8):
            for h in range(per):
                store[b * per + h] = blocks[b][:, h * wb : (h + 1) * wb]
        return jnp.concatenate(blocks, axis=1)


    def slot_send(buf, kind, slot, peer):
        return message(kind, buf.at[slot], buf.at[slot], peer, me)

    def inside(k):
        return (me + k >= 0) & (me + k < n)

    def spread_near(buf, kind, slot, act):
        for k in NEAR:
            @pl.when(inside(k))
            def _():
                act(slot_send(buf, kind, slot, me + k))

    def spread_rest(buf, kind, slot, act):
        @pl.loop(1, n // 2)
        def _(k):
            peer = lax.rem(me + 2 * k, n)
            @pl.when(((peer - me) != 2) & ((peer - me) != -2))
            def _():
                act(slot_send(buf, kind, slot, peer))

    def near_odd(diff):
        return (diff == 1) | (diff == -1) | (diff == -3)

    def arrival(buf, kind, shift, source):
        return message(kind, buf.at[me + shift], buf.at[source + shift], me, source)

    def forward(buf, kind, shift, source):
        slot = source + shift
        return message(kind, buf.at[slot], buf.at[slot], buddy, source, fwd_s.at[kind, source])

    def relay(buf, kind, shift, near):
        @pl.loop(1, n // 2)
        def _(k):
            source = lax.rem(me + n - 2 * k, n)
            diff = source - me
            done = functools.reduce(jnp.logical_or, [diff == d for d in near], False)

            @pl.when(jnp.logical_not(done))
            def _():
                arrival(buf, kind, shift, source).wait_recv()

            @pl.when(jnp.logical_not(near_odd(buddy - source)))
            def _():
                forward(buf, kind, shift, source).start()

    def collect(buf, kind, shift, near):
        @pl.loop(0, n // 2)
        def _(k):
            source = lax.rem(buddy + 2 * k, n)
            diff = source - me
            done = functools.reduce(jnp.logical_or, [diff == d for d in near], False)

            @pl.when(jnp.logical_not(done))
            def _():
                arrival(buf, kind, shift, source).wait_recv()

    def start(copy):
        copy.start()

    def wait_send(copy):
        copy.wait_send()

    lat[me + 2] = mm(regroup(hidden, stk_mine), wd_v[...]).astype(BF)
    hear(3)
    for d in range(4, dims):
        tell(d)
        hear(d)
    spread_near(lat, LAT, me + 2, start)
    spread_rest(lat, LAT, me + 2, start)

    loads[5].wait()
    loads[7].wait()

    @pl.when(me < n - 1)
    def _():
        send_c().wait_recv()

    dec = added(acc_d, future(cbuf, 0, wx_v, (1, 2)))
    own_c = cbuf[0:2, 1 : rows + 1].reshape(fine, ch).astype(F32)
    depth = regroup((own_c + aligned(dec)).astype(BF), dep_mine)
    cgr[me] = mm_nt(depth, wu_v[...]).astype(BF)
    spread_near(cgr, CGR, me, start)

    def block_send(kind, mine, everyone, peer):
        return block(kind, mine.at[peer // rep], everyone.at[me], peer)

    @pl.loop(1, n)
    def _(k):
        block_send(DEP, dep_mine, dep_all, peer_of(k)).start()

    spread_rest(cgr, CGR, me, start)

    @pl.loop(1, n)
    def _(k):
        block_send(STK, stk_mine, stk_all, peer_of(k)).start()

    dep_all[me] = dep_mine[me // rep]
    stk_all[me] = stk_mine[me // rep]

    half = ((level_v[...].astype(F32) - 1.0) * 0.5).reshape(1, ch)
    inverse = 1.0 / half

    def coder(frame, count):
        columns = jnp.concatenate(
            [lat[pl.ds(frame + p, count)].reshape(count * cells, ch) for p in range(3)], axis=1
        )
        squashed = jnp.tanh(mm(columns, wc_v[...]))
        bounded = half * squashed
        sine, cosine = half_turn(bounded)
        codes = ((bounded - sine * cosine * (2.0 / two_pi)) * inverse).astype(BF)
        return codes, (2.0 * sine * sine) * (1.0 - squashed * squashed)

    wc_flip = jnp.concatenate([wc_v[pl.ds((2 - p) * ch, ch)] for p in range(3)], axis=1)

    @pl.when(me < n - 1)
    def _():
        send_n().wait_recv()

    ahead = aligned(past(vbuf, 2, we_v, (0, 1, 2)))

    def moved_exactly(perm, x):
        high = x.astype(BF)
        rest = x - high.astype(F32)
        middle = rest.astype(BF)
        low = (rest - middle.astype(F32)).astype(BF)
        return mm(perm, high) + (mm(perm, middle) + mm(perm, low))

    slopes = [
        moved_exactly(perm_v[0], slope_of(x, s))
        for x, s in ((pre_enc, sig), (ahead, jax.nn.sigmoid(ahead)))
    ]

    lat_near = (-1, -2, 1, 2, 3)
    cgr_near = (1, 2, 3)
    for k in lat_near:
        @pl.when(inside(k))
        def _():
            arrival(lat, LAT, 2, me + k).wait_recv()

    codes, factor = coder(me, 4)
    code_out[...] = codes[0:cells].reshape(code_out.shape)
    relay(lat, LAT, 2, lat_near)

    for k in cgr_near:
        @pl.when(inside(k))
        def _():
            arrival(cgr, CGR, 0, me + k).wait_recv()

    ahead_grad = cgr[pl.ds(me, 4)].reshape(4 * cells, ch).astype(F32) * factor
    later = jnp.concatenate(
        [ahead_grad[p * cells : (p + 2) * cells].astype(BF) for p in range(3)], axis=1
    )
    grad_lat = mm_nt(later, wc_flip).astype(BF)

    deep_grad = mm_nt(grad_lat, wd_v[...])
    deep_rows = [
        jnp.concatenate(
            [
                deep_grad[frame * cells : (frame + 1) * cells, b * ch : (b + 1) * ch]
                for b in range(8)
            ],
            axis=0,
        )
        for frame in range(2)
    ]
    back = perm_v[1]
    for frame in range(2):
        ebuf[2 * frame : 2 * frame + 2, 1 : rows + 1] = (
            mm(back, (deep_rows[frame] * slopes[frame]).astype(BF))
            .astype(BF)
            .reshape(2, rows, width, ch)
        )
    hidden_grad = moved_exactly(back, deep_rows[0])

    collect(lat, LAT, 2, lat_near)
    step = min(n, 16)
    total = n * cells

    @pl.loop(0, n // step)
    def _(k):
        at = k * step
        codes, factor = coder(at, step)
        cod[pl.ds(at, step)] = codes.reshape(step, cells, ch)
        fac[pl.ds(at, step)] = factor.reshape(step, cells, ch)

    all_blocks(DEP, dep_all, n - 1).wait_recv()

    up_part = mm_tn(cod[...].reshape(total, ch), dep_all[...].reshape(total, wb)) * scale
    block_rows = up_mine.shape[1]
    up_mine[...] = up_part.reshape(up_mine.shape)
    up_rows = ch // n
    mine = lax.rem(me, rep)
    my_block = me // rep

    def up_target(k):
        return mine + rep * lax.rem(my_block + k, nb)

    def up_send(peer):
        return block(UPS, up_mine.at[peer * up_rows // block_rows], up_all.at[my_block], peer)

    @pl.loop(1, nb)
    def _(k):
        up_send(up_target(k)).start()

    up_all[my_block] = up_mine[me * up_rows // block_rows]

    def take_rows(buf, at, out):
        count = out.shape[0]
        if count % 8 == 0:
            out[...] = buf[pl.ds(pl.multiple_of(at, 8), count)]
        else:
            for k in range(count):
                out[pl.ds(k, 1)] = buf[pl.ds(at + k, 1)]

    relay(cgr, CGR, 0, cgr_near)
    bck = future(ebuf, 0, we_v, (0, 1, 2))
    vg_out[...] = (hidden_grad + aligned(bck)).astype(BF).reshape(vg_out.shape)
    collect(cgr, CGR, 0, cgr_near)
    pre[2 : n + 2] = (cgr[0:n].astype(F32) * fac[...]).astype(BF)
    long = (n + 2) * cells
    shifted = jnp.concatenate(
        [pre[2 - p : 2 - p + n + 2].reshape(long, ch) for p in range(3)], axis=1
    )
    coarse_all = mm_tn(lat[0 : n + 2].reshape(long, ch), shifted) * scale
    for p in range(3):
        coarse_v[pl.ds(p * ch, ch)] = coarse_all[:, p * ch : (p + 1) * ch]
    take_rows(coarse_v, me * coarse_out.shape[0], coarse_out)
    later_all = jnp.concatenate([pre[2 + p : 2 + p + n].reshape(total, ch) for p in range(3)], axis=1)
    lgr[...] = mm_nt(later_all, wc_flip).astype(BF).reshape(lgr.shape)

    all_blocks(STK, stk_all, n - 1).wait_recv()

    whole_v[0:wb, 0:ch] = (
        mm_tn(stk_all[...].reshape(total, wb), lgr[...].reshape(total, ch)) * scale
    )
    take_rows(whole_v.at[:, pl.ds(0, ch)], mine * down_out.shape[0], down_out)

    @pl.when(me < n - 1)
    def _():
        send_v().wait_send()

    @pl.when(me > 0)
    def _():
        send_c().wait_send()
        send_n().wait_send()

    for buf, kind, shift in ((lat, LAT, 2), (cgr, CGR, 0)):
        spread_near(buf, kind, me + shift, wait_send)
        spread_rest(buf, kind, me + shift, wait_send)

        @pl.loop(1, n // 2)
        def _(k):
            source = lax.rem(me + n - 2 * k, n)

            @pl.when(jnp.logical_not(near_odd(buddy - source)))
            def _():
                forward(buf, kind, shift, source).wait_send()

    all_blocks(DEP, dep_all, n - 1).wait_send()
    all_blocks(STK, stk_all, n - 1).wait_send()
    all_blocks(UPS, up_all, nb - 1).wait_recv()

    up_at = lax.rem(me * up_rows, block_rows)
    for b in range(nb):
        take_rows(up_all.at[b], up_at, up_out.at[:, pl.ds(b * wb, wb)])

    all_blocks(UPS, up_all, nb - 1).wait_send()


def tail(*refs):
    sems = refs[-1]
    count = len(refs) // 2
    copies = [pltpu.make_async_copy(refs[k], refs[count + k], sems.at[k]) for k in range(count)]
    for copy in copies:
        copy.start()
    for copy in copies:
        copy.wait()


def shards(n, vf, ct, we, wd, wc, wu, wx, levels):
    frames, rows, width, ch = vf.shape
    deep = wd.shape[0]
    fine = frames * rows * width
    cells = fine // 8
    wb = max(128, deep // n)
    nb = deep // wb
    up_rows = ch // n
    block_rows = max(8, up_rows)
    scale = 1.0 / math.sqrt(n * fine)
    picks = depth_permutation(rows, width)
    perm = jnp.asarray(np.stack([picks, picks.T]), BF)
    anywhere = pl.BlockSpec(memory_space=pl.ANY)
    results = (
        (vf.shape, BF),
        ((frames // 2, rows // 2, width // 2, ch), BF),
        ((deep // n, ch), F32),
        ((wc.shape[0] // n, ch), F32),
        ((up_rows, deep), F32),
    )
    four = (4, rows + 2, width, ch)
    scratch = [
        pltpu.VMEM((6, rows + 2, width, ch), BF), pltpu.VMEM(four, BF), pltpu.VMEM(four, BF),
        pltpu.VMEM(we.shape, BF), pltpu.VMEM(wx.shape, BF), pltpu.VMEM(wd.shape, BF),
        pltpu.VMEM(wc.shape, BF), pltpu.VMEM(wu.shape, BF), pltpu.VMEM(perm.shape, BF),
        pltpu.VMEM(levels.shape, jnp.int32),
        pltpu.VMEM((n + 5, cells, ch), BF), pltpu.VMEM((n + 3, cells, ch), BF),
        pltpu.VMEM((n, cells, ch), BF), pltpu.VMEM((n, cells, ch), F32),
        pltpu.VMEM((n + 4, cells, ch), BF), pltpu.VMEM((n, cells, ch), BF),
        pltpu.VMEM((nb, cells, wb), BF), pltpu.VMEM((n, cells, wb), BF),
        pltpu.VMEM((nb, cells, wb), BF), pltpu.VMEM((n, cells, wb), BF),
        pltpu.VMEM((ch // block_rows, block_rows, wb), F32),
        pltpu.VMEM((nb, block_rows, wb), F32),
        pltpu.VMEM(wc.shape, F32), pltpu.VMEM((wb, ch), F32),
        pltpu.VMEM((3, fine, ch), F32), pltpu.VMEM((3, fine, ch), F32),
        pltpu.SemaphoreType.DMA((3,)), pltpu.SemaphoreType.DMA((3,)),
        pltpu.SemaphoreType.DMA((2, n)), pltpu.SemaphoreType.DMA((2, n)),
        pltpu.SemaphoreType.DMA((2, n)), pltpu.SemaphoreType.DMA((3,)),
        pltpu.SemaphoreType.DMA((3,)), pltpu.SemaphoreType.DMA((13,)),
        pltpu.SemaphoreType.REGULAR((n.bit_length() - 1,)),
    ]
    held = pl.pallas_call(
        functools.partial(kernel, n, scale),
        out_shape=tuple(pltpu.VMEM(*result) for result in results),
        in_specs=[anywhere] * 9,
        out_specs=(pl.BlockSpec(memory_space=pltpu.VMEM),) * 5,
        scratch_shapes=scratch,
        compiler_params=pltpu.CompilerParams(collective_id=0, has_side_effects=True),
    )(vf, ct, we, wd, wc, wu, wx, levels, perm)
    return pl.pallas_call(
        tail,
        out_shape=tuple(jax.ShapeDtypeStruct(*result) for result in results),
        in_specs=[anywhere] * 5,
        out_specs=(anywhere,) * 5,
        scratch_shapes=[pltpu.SemaphoreType.DMA((5,))],
    )(*[pltpu.with_memory_space_constraint(part, pltpu.VMEM) for part in held])


def solution(mesh):
    placed = (P("tm", "grp", None, None), P("tm", "grp", None, None), P(), P(), P(), P(), P(), P())
    return jax.shard_map(
        functools.partial(shards, mesh.shape["tm"]),
        mesh=mesh,
        in_specs=placed,
        out_specs=(
            P("tm", "grp", None, None),
            P("tm", "grp", None, None),
            P(("grp", "tm"), None),
            P(("grp", "tm"), None),
            P(("grp", "tm"), None),
        ),
        check_vma=False,
    )
```

```python
import functools
import math

import jax
import jax.numpy as jnp
import numpy as np
from jax import lax
from jax.experimental import pallas as pl
from jax.experimental.pallas import tpu as pltpu
from jax.sharding import PartitionSpec as P

two_pi = 2.0 * math.pi
BF = jnp.bfloat16
F32 = jnp.float32
MESH = pl.DeviceIdType.MESH

HALO_V, HALO_C, HALO_N = 0, 1, 2
LAT, CGR = 0, 1
BUDDY = 2
STK, DEP, UPS = 4, 5, 6

SINE = [(-1.0) ** k / math.factorial(2 * k + 1) for k in range(7)]
COSINE = [(-1.0) ** k / math.factorial(2 * k) for k in range(7)]

def mm(a, b):
    return jnp.dot(a, b, preferred_element_type=F32)


def mm_nt(a, b):
    return lax.dot_general(a, b, (((1,), (1,)), ((), ())), preferred_element_type=F32)


def mm_tn(a, b):
    return lax.dot_general(a, b, (((0,), (0,)), ((), ())), preferred_element_type=F32)


def half_turn(x):
    angle = (x - jnp.round(x)) * math.pi
    square = angle * angle
    sine, cosine = SINE[-1], COSINE[-1]
    for a, b in zip(SINE[-2::-1], COSINE[-2::-1]):
        sine = sine * square + a
        cosine = cosine * square + b
    return sine * angle, cosine


def depth_permutation(rows, cols):
    order = np.arange(2 * rows * cols).reshape(2, rows // 2, 2, cols // 2, 2)
    order = order.transpose(0, 2, 4, 1, 3).reshape(-1)
    picks = np.zeros((order.size, order.size), np.float32)
    picks[np.arange(order.size), order] = 1.0
    return picks


def kernel(
    n, scale, vf, ct, we, wd, wc, wu, wx, levels, perm,
    vg_out, code_out, down_out, coarse_out, up_out,
    vg_w, code_w, down_w, coarse_w, up_w, lat_turned,
    vbuf, cbuf, ebuf, we_v, wx_v, wd_v, wc_v, wu_v, perm_v, level_v,
    lat, cgr, near, cod, fac, pre, lgr, stk_mine, stk_all, dep_mine, dep_all, up_mine, up_all, up_wide, coarse_v, whole_v,
    acc_e, acc_d, hal_s, hal_r, msg_r, near_s, near_r, all_s, all_r, load_sem, out_sem, met,
):
    frames, rows, width, ch = vf.shape
    fine = frames * rows * width
    cells = fine // 8
    nb, _, wb = stk_mine.shape
    rep = n // nb
    me = lax.axis_index("tm")

    def peer_of(k):
        return lax.rem(me + k, n)

    odd = lax.rem(me, 2)
    buddy = me + 1 - 2 * odd
    other = me - 1 + 2 * odd
    has_other = (other >= 0) & (other < n)
    dims = n.bit_length() - 1

    def partner(d):
        return me + (1 - 2 * lax.rem(me // 2**d, 2)) * 2**d

    barrier = pltpu.get_barrier_semaphore()
    for d in range(dims):
        pl.semaphore_signal(barrier, inc=1, device_id={"tm": partner(d)}, device_id_type=MESH)

    @pl.when(has_other)
    def _():
        pl.semaphore_signal(barrier, inc=1, device_id={"tm": other}, device_id_type=MESH)

    def tell(d):
        if d < dims:
            pl.semaphore_signal(
                met.at[d], inc=1, device_id={"tm": partner(d)}, device_id_type=MESH
            )

    def hear(d):
        if d < dims:
            pl.semaphore_wait(met.at[d], 1)

    inner = pl.ds(1, rows)
    third = we.shape[0] // 3
    loads = [
        pltpu.make_async_copy(vf, vbuf.at[2:4, inner], load_sem.at[0]),
        pltpu.make_async_copy(ct, cbuf.at[0:2, inner], load_sem.at[1]),
    ]
    for k, (at, count) in enumerate(((2 * third, third), (0, 2 * third))):
        span = pl.ds(at, count)
        loads.append(pltpu.make_async_copy(we.at[span], we_v.at[span], load_sem.at[2 + 2 * k]))
        loads.append(pltpu.make_async_copy(wx.at[span], wx_v.at[span], load_sem.at[3 + 2 * k]))
    small = [
        pltpu.make_async_copy(src, dst, load_sem.at[6 + k])
        for k, (src, dst) in enumerate(
            ((perm, perm_v), (wd, wd_v), (wu, wu_v), (wc, wc_v), (levels, level_v))
        )
    ]
    for load in loads + small:
        load.start()

    def halo(kind, src, dst, peer):
        return pltpu.make_async_remote_copy(
            src_ref=src, dst_ref=dst, send_sem=hal_s.at[kind], recv_sem=hal_r.at[kind],
            device_id={"tm": peer}, device_id_type=MESH,
        )

    def block(kind, src, dst, peer, receives=None, sends=None):
        return pltpu.make_async_remote_copy(
            src_ref=src, dst_ref=dst,
            send_sem=all_s.at[kind] if sends is None else sends,
            recv_sem=all_r.at[kind] if receives is None else receives,
            device_id={"tm": peer}, device_id_type=MESH,
        )

    def all_blocks(kind, buf, count):
        return block(kind, buf.at[pl.ds(0, count)], buf.at[pl.ds(0, count)], buddy)

    def send_v():
        return halo(HALO_V, vf, vbuf.at[0:2, inner], me + 1)

    def send_c():
        return halo(HALO_C, ct, cbuf.at[2:4, inner], me - 1)

    def send_n():
        return halo(HALO_N, vf, vbuf.at[4:6, inner], me - 1)

    for buf in (vbuf, cbuf, ebuf):
        edge = jnp.zeros((buf.shape[0], 1, width, ch), BF)
        buf[:, 0:1] = edge
        buf[:, rows + 1 : rows + 2] = edge
    blank = jnp.zeros((2, rows, width, ch), BF)

    @pl.when(me == 0)
    def _():
        vbuf[0:2, 1 : rows + 1] = blank

    @pl.when(me == n - 1)
    def _():
        cbuf[2:4, 1 : rows + 1] = blank
        vbuf[4:6, 1 : rows + 1] = blank

    lat[0:2] = jnp.zeros((2, cells, ch), BF)
    lat[n + 2 : n + 5] = jnp.zeros((3, cells, ch), BF)
    for k in (1, 2, 3):
        @pl.when(me + k >= n)
        def _():
            near[k - 1] = jnp.zeros((cells, ch), BF)

    fac[n : n + 3] = jnp.zeros((3, cells, ch), F32)
    pre[0:2] = jnp.zeros((2, cells, ch), BF)
    pre[n + 2 : n + 4] = jnp.zeros((2, cells, ch), BF)

    pl.semaphore_wait(barrier, jnp.where(has_other, dims + 1, dims))
    tell(0)

    @pl.when(me < n - 1)
    def _():
        send_v().start()

    @pl.when(me > 0)
    def _():
        send_c().start()
        send_n().start()

    def taps(buf, at):
        return jnp.concatenate(
            [buf[at : at + 2, q : q + rows].reshape(fine, ch) for q in range(3)], axis=1
        )

    def past(buf, at, weight, parts):
        left = jnp.concatenate([taps(buf, at + p) for p in parts], axis=1)
        out = []
        for r in range(3):
            right = jnp.concatenate(
                [
                    weight[pl.ds(((3 * p + q) * 3 + r) * ch, ch)]
                    for p in parts
                    for q in range(3)
                ],
                axis=0,
            )
            out.append(mm(left, right))
        return out

    def future(buf, at, weight, parts):
        left = jnp.concatenate([taps(buf, at + p) for p in parts], axis=1)
        out = []
        for r in range(3):
            right = jnp.concatenate(
                [
                    weight[pl.ds((((2 - p) * 3 + 2 - q) * 3 + 2 - r) * ch, ch)]
                    for p in parts
                    for q in range(3)
                ],
                axis=1,
            )
            out.append(mm_nt(left, right))
        return out

    def keep(acc, parts):
        for r in range(3):
            acc[r] = parts[r]

    def added(acc, parts):
        return [acc[r] + parts[r] for r in range(3)]

    lane = lax.broadcasted_iota(jnp.int32, (fine // width, width, ch), 1)

    def aligned(parts):
        a, b, c = [x.reshape(fine // width, width, ch) for x in parts]
        a = jnp.where(lane == 0, 0.0, pltpu.roll(a, 1, 1))
        c = jnp.where(lane == width - 1, 0.0, pltpu.roll(c, width - 1, 1))
        return (a + b + c).reshape(fine, ch)

    hear(0)
    tell(1)

    loads[0].wait()
    loads[2].wait()
    keep(acc_e, past(vbuf, 0, we_v, (2,)))
    hear(1)
    tell(2)
    loads[1].wait()
    loads[3].wait()
    keep(acc_d, future(cbuf, 0, wx_v, (0,)))
    hear(2)
    tell(3)
    loads[4].wait()

    @pl.when(me > 0)
    def _():
        send_v().wait_recv()

    enc = added(acc_e, past(vbuf, 0, we_v, (1, 0)))
    pre_enc = aligned(enc)
    sig = jax.nn.sigmoid(pre_enc)
    own = vbuf[2:4, 1 : rows + 1].reshape(fine, ch).astype(F32)
    hidden = (own + pre_enc * sig).astype(BF)

    def slope_of(x, s):
        return s * (1.0 + x * (1.0 - s))

    for load in small:
        load.wait()

    def regroup(field, store):
        moved = mm(perm_v[0], field)
        blocks = [moved[b * cells : (b + 1) * cells].astype(BF) for b in range(8)]
        per = nb // 8
        for b in range(8):
            for h in range(per):
                store[b * per + h] = blocks[b][:, h * wb : (h + 1) * wb]
        return jnp.concatenate(blocks, axis=1)

    half_n = n // 2

    def parity_send(buf, kind, slot, k):
        peer = lax.rem(me + 2 * k, n)
        return block(kind, buf.at[slot], buf.at[slot], peer, msg_r.at[kind, me // 2])

    def buddy_send(buf, kind, slot):
        return block(BUDDY + kind, buf.at[slot], buf.at[slot], buddy)

    def near_send(k):
        return block(
            CGR, cgr.at[me], near.at[k - 1], me - k, near_r.at[k - 1], near_s.at[k - 1]
        )

    def arrival(buf, kind, slot, source):
        return block(kind, buf.at[slot], buf.at[slot], buddy, msg_r.at[kind, source // 2])

    def inside(k):
        return (me + k >= 0) & (me + k < n)

    def spread(buf, kind, slot):
        buddy_send(buf, kind, slot).start()

        @pl.loop(1, half_n)
        def _(k):
            parity_send(buf, kind, slot, k).start()

    def relay(buf, kind, shift):
        @pl.loop(1, half_n)
        def _(k):
            source = lax.rem(me + n - 2 * k, n)
            slot = source + shift
            arrival(buf, kind, slot, source).wait_recv()
            block(BUDDY + kind, buf.at[slot], buf.at[slot], buddy).start()

    lat[me + 2] = mm(regroup(hidden, stk_mine), wd_v[...]).astype(BF)
    hear(3)
    for d in range(4, dims):
        tell(d)
        hear(d)
    spread(lat, LAT, me + 2)

    loads[5].wait()

    @pl.when(me < n - 1)
    def _():
        send_c().wait_recv()

    dec = added(acc_d, future(cbuf, 0, wx_v, (1, 2)))
    own_c = cbuf[0:2, 1 : rows + 1].reshape(fine, ch).astype(F32)
    depth = regroup((own_c + aligned(dec)).astype(BF), dep_mine)

    def block_send(kind, mine, everyone, peer):
        return block(kind, mine.at[peer // rep], everyone.at[me], peer)

    @pl.loop(1, n)
    def _(k):
        block_send(DEP, dep_mine, dep_all, peer_of(k)).start()

    cgr[me] = mm_nt(depth, wu_v[...]).astype(BF)

    for k in (1, 2, 3):
        @pl.when(inside(-k))
        def _():
            near_send(k).start()

    spread(cgr, CGR, me)

    dep_all[me] = dep_mine[me // rep]
    stk_all[me] = stk_mine[me // rep]

    def give(src, dst, k):
        return pltpu.make_async_copy(src, dst, out_sem.at[k])

    half = ((level_v[...].astype(F32) - 1.0) * 0.5).reshape(1, ch)
    inverse = 1.0 / half

    def coder(frame, count):
        columns = jnp.concatenate(
            [lat[pl.ds(frame + p, count)].reshape(count * cells, ch) for p in range(3)], axis=1
        )
        squashed = jnp.tanh(mm(columns, wc_v[...]))
        bounded = half * squashed
        sine, cosine = half_turn(bounded)
        codes = ((bounded - sine * cosine * (2.0 / two_pi)) * inverse).astype(BF)
        return codes, (2.0 * sine * sine) * (1.0 - squashed * squashed)

    wc_flip = jnp.concatenate([wc_v[pl.ds((2 - p) * ch, ch)] for p in range(3)], axis=1)

    @pl.when(me < n - 1)
    def _():
        send_n().wait_recv()

    ahead = aligned(past(vbuf, 2, we_v, (0, 1, 2)))

    relay(lat, LAT, 2)

    @pl.loop(1, n)
    def _(k):
        block_send(STK, stk_mine, stk_all, peer_of(k)).start()

    def moved(perm, x):
        high = x.astype(BF)
        rest = (x - high.astype(F32)).astype(BF)
        return mm(perm, high) + mm(perm, rest)

    slopes = [
        moved(perm_v[0], slope_of(x, s))
        for x, s in ((pre_enc, sig), (ahead, jax.nn.sigmoid(ahead)))
    ]

    all_blocks(BUDDY + LAT, lat, half_n).wait_recv()
    step = min(n, 16)
    total = n * cells

    @pl.loop(0, n // step)
    def _(k):
        at = k * step
        codes, factor = coder(at, step)
        cod[pl.ds(at, step)] = codes.reshape(step, cells, ch)
        fac[pl.ds(at, step)] = factor.reshape(step, cells, ch)

    code_w[...] = cod[me].reshape(code_w.shape)
    code_out_copy = give(code_w, code_out, 0)
    code_out_copy.start()
    codes_turned = cod[...].reshape(total, ch).T
    lat_turned[...] = lat[0 : n + 2].reshape((n + 2) * cells, ch).T

    all_blocks(DEP, dep_all, n - 1).wait_recv()

    up_part = mm(codes_turned, dep_all[...].reshape(total, wb)) * scale
    block_rows = up_mine.shape[1]
    up_mine[...] = up_part.astype(BF).reshape(up_mine.shape)
    up_rows = ch // n
    mine = lax.rem(me, rep)
    my_block = me // rep

    def up_target(k):
        return mine + rep * lax.rem(my_block + k, nb)

    direct = block_rows == up_rows
    blocks_in = up_out if direct else up_all

    def up_send(peer):
        return block(UPS, up_mine.at[peer * up_rows // block_rows], blocks_in.at[my_block], peer)

    @pl.loop(1, nb)
    def _(k):
        up_send(up_target(k)).start()

    own_copy = give(up_mine.at[me * up_rows // block_rows], blocks_in.at[my_block], 4)
    own_copy.start()

    def take_rows(buf, at, out):
        count = out.shape[0]
        if count % 8 == 0:
            out[...] = buf[pl.ds(pl.multiple_of(at, 8), count)]
        else:
            for k in range(count):
                out[pl.ds(k, 1)] = buf[pl.ds(at + k, 1)]

    for k in (1, 2, 3):
        @pl.when(inside(k))
        def _():
            near_send(k).wait_recv()

    near_grads = jnp.concatenate([cgr[me], *[near[k] for k in range(3)]], axis=0).astype(F32)
    ahead_grad = near_grads * fac[pl.ds(me, 4)].reshape(4 * cells, ch)
    later = jnp.concatenate(
        [ahead_grad[p * cells : (p + 2) * cells].astype(BF) for p in range(3)], axis=1
    )
    grad_lat = mm_nt(later, wc_flip).astype(BF)

    deep_grad = mm_nt(grad_lat, wd_v[...])
    deep_rows = [
        jnp.concatenate(
            [
                deep_grad[frame * cells : (frame + 1) * cells, b * ch : (b + 1) * ch]
                for b in range(8)
            ],
            axis=0,
        )
        for frame in range(2)
    ]
    back = perm_v[1]
    for frame in range(2):
        ebuf[2 * frame : 2 * frame + 2, 1 : rows + 1] = (
            mm(back, (deep_rows[frame] * slopes[frame]).astype(BF))
            .astype(BF)
            .reshape(2, rows, width, ch)
        )
    hidden_grad = moved(back, deep_rows[0])

    bck = future(ebuf, 0, we_v, (0, 1, 2))
    vg_w[...] = (hidden_grad + aligned(bck)).astype(BF).reshape(vg_w.shape)
    vg_copy = give(vg_w, vg_out, 1)
    vg_copy.start()
    relay(cgr, CGR, 0)
    all_blocks(BUDDY + CGR, cgr, half_n).wait_recv()
    pre[2 : n + 2] = (cgr[0:n].astype(F32) * fac[0:n]).astype(BF)
    long = (n + 2) * cells
    coarse_rows = coarse_w.shape[0]
    piece = math.gcd(coarse_rows, ch)
    if piece % 16 == 0:
        for k in range(coarse_rows // piece):
            at = me * coarse_rows + k * piece
            left = lat_turned[pl.ds(pl.multiple_of(lax.rem(at, ch), piece), piece)]
            right = pre[pl.ds(2 - at // ch, n + 2)].reshape(long, ch)
            coarse_w[k * piece : (k + 1) * piece] = mm(left, right) * scale
    else:
        for p in range(3):
            coarse_v[pl.ds(p * ch, ch)] = (
                mm(lat_turned[...], pre[2 - p : 2 - p + n + 2].reshape(long, ch)) * scale
            )
        take_rows(coarse_v, me * coarse_rows, coarse_w)
    coarse_copy = give(coarse_w, coarse_out, 2)
    coarse_copy.start()
    later_all = jnp.concatenate([pre[2 + p : 2 + p + n].reshape(total, ch) for p in range(3)], axis=1)
    lgr[...] = mm_nt(later_all, wc_flip).astype(BF).reshape(lgr.shape)

    all_blocks(STK, stk_all, n - 1).wait_recv()

    whole_v[...] = (
        mm_tn(stk_all[...].reshape(total, wb), lgr[...].reshape(total, ch)) * scale
    )
    take_rows(whole_v, mine * down_out.shape[0], down_w)
    down_copy = give(down_w, down_out, 3)
    down_copy.start()

    @pl.when(me < n - 1)
    def _():
        send_v().wait_send()

    @pl.when(me > 0)
    def _():
        send_c().wait_send()
        send_n().wait_send()

    all_blocks(LAT, lat, half_n - 1).wait_send()
    all_blocks(CGR, cgr, half_n - 1).wait_send()
    all_blocks(BUDDY + LAT, lat, half_n).wait_send()
    all_blocks(BUDDY + CGR, cgr, half_n).wait_send()
    for k in (1, 2, 3):
        @pl.when(inside(-k))
        def _():
            near_send(k).wait_send()

    all_blocks(DEP, dep_all, n - 1).wait_send()
    all_blocks(STK, stk_all, n - 1).wait_send()
    for copy in (code_out_copy, vg_copy, coarse_copy, down_copy, own_copy):
        copy.wait()
    all_blocks(UPS, blocks_in, nb - 1).wait_recv()
    all_blocks(UPS, blocks_in, nb - 1).wait_send()
    if not direct:
        up_wide[...] = up_all[...].astype(F32)
        for b in range(nb):
            take_rows(up_wide.at[b], lax.rem(me * up_rows, block_rows), up_w.at[b])
        up_copy = give(up_w, up_out, 0)
        up_copy.start()
        up_copy.wait()


def tail(vg, code, down, coarse, up, vg_out, code_out, down_out, coarse_out, up_out, wide, sems):
    nb, _, wb = up.shape
    pairs = ((vg, vg_out), (code, code_out), (down, down_out), (coarse, coarse_out), (wide, up_out))
    copies = [pltpu.make_async_copy(src, dst, sems.at[k]) for k, (src, dst) in enumerate(pairs)]
    for copy in copies[:4]:
        copy.start()
    for b in range(nb):
        wide[:, b * wb : (b + 1) * wb] = up[b].astype(F32)
    copies[4].start()
    for copy in copies:
        copy.wait()


def shards(n, vf, ct, we, wd, wc, wu, wx, levels):
    frames, rows, width, ch = vf.shape
    deep = wd.shape[0]
    fine = frames * rows * width
    cells = fine // 8
    wb = max(128, deep // n)
    nb = deep // wb
    up_rows = ch // n
    block_rows = max(8, up_rows)
    scale = 1.0 / math.sqrt(n * fine)
    picks = depth_permutation(rows, width)
    perm = jnp.asarray(np.stack([picks, picks.T]), BF)
    anywhere = pl.BlockSpec(memory_space=pl.ANY)
    results = (
        (vf.shape, BF),
        ((frames // 2, rows // 2, width // 2, ch), BF),
        ((deep // n, ch), F32),
        ((wc.shape[0] // n, ch), F32),
        ((up_rows, deep), F32),
    )
    four = (4, rows + 2, width, ch)
    held_shapes = (
        results[0],
        results[1],
        results[2],
        results[3],
        ((nb, up_rows, wb), BF if block_rows == up_rows else F32),
    )
    scratch = [
        pltpu.VMEM(vf.shape, BF), pltpu.VMEM(results[1][0], BF), pltpu.VMEM(results[2][0], F32), pltpu.VMEM(results[3][0], F32),
        pltpu.VMEM((nb, up_rows, wb), F32), pltpu.VMEM((ch, (n + 2) * cells), BF),
        pltpu.VMEM((6, rows + 2, width, ch), BF), pltpu.VMEM(four, BF), pltpu.VMEM(four, BF),
        pltpu.VMEM(we.shape, BF), pltpu.VMEM(wx.shape, BF), pltpu.VMEM(wd.shape, BF),
        pltpu.VMEM(wc.shape, BF), pltpu.VMEM(wu.shape, BF), pltpu.VMEM(perm.shape, BF),
        pltpu.VMEM(levels.shape, jnp.int32),
        pltpu.VMEM((n + 5, cells, ch), BF), pltpu.VMEM((n, cells, ch), BF), pltpu.VMEM((3, cells, ch), BF),
        pltpu.VMEM((n, cells, ch), BF), pltpu.VMEM((n + 3, cells, ch), F32),
        pltpu.VMEM((n + 4, cells, ch), BF), pltpu.VMEM((n, cells, ch), BF),
        pltpu.VMEM((nb, cells, wb), BF), pltpu.VMEM((n, cells, wb), BF),
        pltpu.VMEM((nb, cells, wb), BF), pltpu.VMEM((n, cells, wb), BF),
        pltpu.VMEM((ch // block_rows, block_rows, wb), BF),
        pltpu.VMEM((nb, block_rows, wb), BF), pltpu.VMEM((nb, block_rows, wb), F32),
        pltpu.VMEM(wc.shape, F32), pltpu.VMEM((wb, ch), F32),
        pltpu.VMEM((3, fine, ch), F32), pltpu.VMEM((3, fine, ch), F32),
        pltpu.SemaphoreType.DMA((3,)), pltpu.SemaphoreType.DMA((3,)),
        pltpu.SemaphoreType.DMA((2, n // 2)), pltpu.SemaphoreType.DMA((3,)),
        pltpu.SemaphoreType.DMA((3,)), pltpu.SemaphoreType.DMA((7,)),
        pltpu.SemaphoreType.DMA((7,)), pltpu.SemaphoreType.DMA((11,)),
        pltpu.SemaphoreType.DMA((5,)),
        pltpu.SemaphoreType.REGULAR((n.bit_length() - 1,)),
    ]
    held = pl.pallas_call(
        functools.partial(kernel, n, scale),
        out_shape=tuple(pltpu.VMEM(*shape) for shape in held_shapes),
        in_specs=[anywhere] * 9,
        out_specs=(anywhere,) * 5,
        scratch_shapes=scratch,
        compiler_params=pltpu.CompilerParams(collective_id=0, has_side_effects=True),
    )(vf, ct, we, wd, wc, wu, wx, levels, perm)
    return pl.pallas_call(
        tail,
        out_shape=tuple(jax.ShapeDtypeStruct(*result) for result in results),
        in_specs=[anywhere] * 4 + [pl.BlockSpec(memory_space=pltpu.VMEM)],
        out_specs=(anywhere,) * 5,
        scratch_shapes=[pltpu.VMEM((up_rows, deep), F32), pltpu.SemaphoreType.DMA((5,))],
    )(*[pltpu.with_memory_space_constraint(part, pltpu.VMEM) for part in held])


def solution(mesh):
    placed = (P("tm", "grp", None, None), P("tm", "grp", None, None), P(), P(), P(), P(), P(), P())
    return jax.shard_map(
        functools.partial(shards, mesh.shape["tm"]),
        mesh=mesh,
        in_specs=placed,
        out_specs=(
            P("tm", "grp", None, None),
            P("tm", "grp", None, None),
            P(("grp", "tm"), None),
            P(("grp", "tm"), None),
            P(("grp", "tm"), None),
        ),
        check_vma=False,
    )
```

```python
import functools
import math

import jax
import jax.numpy as jnp
import numpy as np
from jax import lax
from jax.experimental import pallas as pl
from jax.experimental.pallas import tpu as pltpu
from jax.sharding import PartitionSpec as P

two_pi = 2.0 * math.pi
BF = jnp.bfloat16
F32 = jnp.float32
MESH = pl.DeviceIdType.MESH

HALO_V, HALO_C, HALO_N = 0, 1, 2
LAT, CGR = 0, 1
BUDDY = 2
STK, DEP, UPS = 4, 5, 6

SINE = [(-1.0) ** k / math.factorial(2 * k + 1) for k in range(7)]
COSINE = [(-1.0) ** k / math.factorial(2 * k) for k in range(7)]

def mm(a, b):
    return jnp.dot(a, b, preferred_element_type=F32)


def mm_nt(a, b):
    return lax.dot_general(a, b, (((1,), (1,)), ((), ())), preferred_element_type=F32)


def mm_tn(a, b):
    return lax.dot_general(a, b, (((0,), (0,)), ((), ())), preferred_element_type=F32)


def half_turn(x):
    angle = (x - jnp.round(x)) * math.pi
    square = angle * angle
    sine, cosine = SINE[-1], COSINE[-1]
    for a, b in zip(SINE[-2::-1], COSINE[-2::-1]):
        sine = sine * square + a
        cosine = cosine * square + b
    return sine * angle, cosine


def depth_permutation(rows, cols):
    order = np.arange(2 * rows * cols).reshape(2, rows // 2, 2, cols // 2, 2)
    order = order.transpose(0, 2, 4, 1, 3).reshape(-1)
    picks = np.zeros((order.size, order.size), np.float32)
    picks[np.arange(order.size), order] = 1.0
    return picks


def kernel(
    n, scale, vf, ct, we, wd, wc, wu, wx, levels, perm,
    vg_out, code_out, down_out, coarse_out, up_out,
    vg_w, code_w, down_w, coarse_w, up_w, lat_turned,
    vbuf, cbuf, ebuf, we_v, wx_v, wd_v, wc_v, wu_v, perm_v, level_v,
    lat, cgr, near, cod, fac, pre, lgr, stk_mine, stk_all, dep_mine, dep_all, up_mine, up_all, up_wide, coarse_v, whole_v,
    acc_e, acc_d, hal_s, hal_r, msg_r, near_s, near_r, all_s, all_r, load_sem, out_sem, met,
):
    frames, rows, width, ch = vf.shape
    fine = frames * rows * width
    cells = fine // 8
    nb, _, wb = stk_mine.shape
    rep = n // nb
    me = lax.axis_index("tm")

    def peer_of(k):
        return lax.rem(me + k, n)

    odd = lax.rem(me, 2)
    buddy = me + 1 - 2 * odd
    other = me - 1 + 2 * odd
    has_other = (other >= 0) & (other < n)
    dims = n.bit_length() - 1

    def partner(d):
        return me + (1 - 2 * lax.rem(me // 2**d, 2)) * 2**d

    barrier = pltpu.get_barrier_semaphore()
    for d in range(dims):
        pl.semaphore_signal(barrier, inc=1, device_id={"tm": partner(d)}, device_id_type=MESH)

    @pl.when(has_other)
    def _():
        pl.semaphore_signal(barrier, inc=1, device_id={"tm": other}, device_id_type=MESH)

    def tell(d):
        if d < dims:
            pl.semaphore_signal(
                met.at[d], inc=1, device_id={"tm": partner(d)}, device_id_type=MESH
            )

    def hear(d):
        if d < dims:
            pl.semaphore_wait(met.at[d], 1)

    inner = pl.ds(1, rows)
    third = we.shape[0] // 3
    loads = [
        pltpu.make_async_copy(vf, vbuf.at[2:4, inner], load_sem.at[0]),
        pltpu.make_async_copy(ct, cbuf.at[0:2, inner], load_sem.at[1]),
    ]
    for k, (at, count) in enumerate(((2 * third, third), (0, 2 * third))):
        span = pl.ds(at, count)
        loads.append(pltpu.make_async_copy(we.at[span], we_v.at[span], load_sem.at[2 + 2 * k]))
        loads.append(pltpu.make_async_copy(wx.at[span], wx_v.at[span], load_sem.at[3 + 2 * k]))
    small = [
        pltpu.make_async_copy(src, dst, load_sem.at[6 + k])
        for k, (src, dst) in enumerate(
            ((perm, perm_v), (wd, wd_v), (wu, wu_v), (wc, wc_v), (levels, level_v))
        )
    ]
    for load in loads + small:
        load.start()

    def halo(kind, src, dst, peer):
        return pltpu.make_async_remote_copy(
            src_ref=src, dst_ref=dst, send_sem=hal_s.at[kind], recv_sem=hal_r.at[kind],
            device_id={"tm": peer}, device_id_type=MESH,
        )

    def block(kind, src, dst, peer, receives=None, sends=None):
        return pltpu.make_async_remote_copy(
            src_ref=src, dst_ref=dst,
            send_sem=all_s.at[kind] if sends is None else sends,
            recv_sem=all_r.at[kind] if receives is None else receives,
            device_id={"tm": peer}, device_id_type=MESH,
        )

    def all_blocks(kind, buf, count):
        return block(kind, buf.at[pl.ds(0, count)], buf.at[pl.ds(0, count)], buddy)

    def send_v():
        return halo(HALO_V, vbuf.at[2:4, inner], vbuf.at[0:2, inner], me + 1)

    def send_c():
        return halo(HALO_C, ct, cbuf.at[2:4, inner], me - 1)

    def send_n():
        return halo(HALO_N, vf, vbuf.at[4:6, inner], me - 1)

    for buf in (vbuf, cbuf, ebuf):
        edge = jnp.zeros((buf.shape[0], 1, width, ch), BF)
        buf[:, 0:1] = edge
        buf[:, rows + 1 : rows + 2] = edge
    blank = jnp.zeros((2, rows, width, ch), BF)

    @pl.when(me == 0)
    def _():
        vbuf[0:2, 1 : rows + 1] = blank

    @pl.when(me == n - 1)
    def _():
        cbuf[2:4, 1 : rows + 1] = blank
        vbuf[4:6, 1 : rows + 1] = blank

    lat[0:2] = jnp.zeros((2, cells, ch), BF)
    lat[n + 2 : n + 5] = jnp.zeros((3, cells, ch), BF)
    for k in (1, 2, 3):
        @pl.when(me + k >= n)
        def _():
            near[k - 1] = jnp.zeros((cells, ch), BF)

    fac[n : n + 3] = jnp.zeros((3, cells, ch), F32)
    pre[0:2] = jnp.zeros((2, cells, ch), BF)
    pre[n + 2 : n + 4] = jnp.zeros((2, cells, ch), BF)

    pl.semaphore_wait(barrier, jnp.where(has_other, dims + 1, dims))
    tell(0)

    loads[0].wait()

    @pl.when(me < n - 1)
    def _():
        send_v().start()

    @pl.when(me > 0)
    def _():
        send_c().start()
        send_n().start()

    def taps(buf, at):
        return jnp.concatenate(
            [buf[at : at + 2, q : q + rows].reshape(fine, ch) for q in range(3)], axis=1
        )

    def past(buf, at, weight, parts):
        left = jnp.concatenate([taps(buf, at + p) for p in parts], axis=1)
        out = []
        for r in range(3):
            right = jnp.concatenate(
                [
                    weight[pl.ds(((3 * p + q) * 3 + r) * ch, ch)]
                    for p in parts
                    for q in range(3)
                ],
                axis=0,
            )
            out.append(mm(left, right))
        return out

    def future(buf, at, weight, parts):
        left = jnp.concatenate([taps(buf, at + p) for p in parts], axis=1)
        out = []
        for r in range(3):
            right = jnp.concatenate(
                [
                    weight[pl.ds((((2 - p) * 3 + 2 - q) * 3 + 2 - r) * ch, ch)]
                    for p in parts
                    for q in range(3)
                ],
                axis=1,
            )
            out.append(mm_nt(left, right))
        return out

    def keep(acc, parts):
        for r in range(3):
            acc[r] = parts[r]

    def added(acc, parts):
        return [acc[r] + parts[r] for r in range(3)]

    lane = lax.broadcasted_iota(jnp.int32, (fine // width, width, ch), 1)

    def aligned(parts):
        a, b, c = [x.reshape(fine // width, width, ch) for x in parts]
        a = jnp.where(lane == 0, 0.0, pltpu.roll(a, 1, 1))
        c = jnp.where(lane == width - 1, 0.0, pltpu.roll(c, width - 1, 1))
        return (a + b + c).reshape(fine, ch)

    hear(0)
    tell(1)

    loads[2].wait()
    keep(acc_e, past(vbuf, 0, we_v, (2,)))
    hear(1)
    tell(2)
    loads[1].wait()
    loads[3].wait()
    keep(acc_d, future(cbuf, 0, wx_v, (0,)))
    hear(2)
    tell(3)
    loads[4].wait()

    @pl.when(me > 0)
    def _():
        send_v().wait_recv()

    enc = added(acc_e, past(vbuf, 0, we_v, (1, 0)))
    pre_enc = aligned(enc)
    sig = jax.nn.sigmoid(pre_enc)
    own = vbuf[2:4, 1 : rows + 1].reshape(fine, ch).astype(F32)
    hidden = (own + pre_enc * sig).astype(BF)

    def slope_of(x, s):
        return s * (1.0 + x * (1.0 - s))

    for load in small:
        load.wait()

    def regroup(field, store):
        moved = mm(perm_v[0], field)
        blocks = [moved[b * cells : (b + 1) * cells].astype(BF) for b in range(8)]
        per = nb // 8
        for b in range(8):
            for h in range(per):
                store[b * per + h] = blocks[b][:, h * wb : (h + 1) * wb]
        return jnp.concatenate(blocks, axis=1)

    half_n = n // 2

    def parity_send(buf, kind, slot, k):
        peer = lax.rem(me + 2 * k, n)
        return block(kind, buf.at[slot], buf.at[slot], peer, msg_r.at[kind, me // 2])

    def buddy_send(buf, kind, slot):
        return block(BUDDY + kind, buf.at[slot], buf.at[slot], buddy)

    def near_send(k):
        return block(
            CGR, cgr.at[me], near.at[k - 1], me - k, near_r.at[k - 1], near_s.at[k - 1]
        )

    def arrival(buf, kind, slot, source):
        return block(kind, buf.at[slot], buf.at[slot], buddy, msg_r.at[kind, source // 2])

    def inside(k):
        return (me + k >= 0) & (me + k < n)

    def spread(buf, kind, slot):
        buddy_send(buf, kind, slot).start()

        @pl.loop(1, half_n)
        def _(k):
            parity_send(buf, kind, slot, k).start()

    def relay(buf, kind, shift):
        @pl.loop(1, half_n)
        def _(k):
            source = lax.rem(me + n - 2 * k, n)
            slot = source + shift
            arrival(buf, kind, slot, source).wait_recv()
            block(BUDDY + kind, buf.at[slot], buf.at[slot], buddy).start()

    lat[me + 2] = mm(regroup(hidden, stk_mine), wd_v[...]).astype(BF)
    hear(3)
    for d in range(4, dims):
        tell(d)
        hear(d)
    spread(lat, LAT, me + 2)

    loads[5].wait()

    @pl.when(me < n - 1)
    def _():
        send_c().wait_recv()

    dec = added(acc_d, future(cbuf, 0, wx_v, (1, 2)))
    own_c = cbuf[0:2, 1 : rows + 1].reshape(fine, ch).astype(F32)
    depth = regroup((own_c + aligned(dec)).astype(BF), dep_mine)

    def block_send(kind, mine, everyone, peer):
        return block(kind, mine.at[peer // rep], everyone.at[me], peer)

    @pl.loop(1, n)
    def _(k):
        block_send(DEP, dep_mine, dep_all, peer_of(k)).start()

    cgr[me] = mm_nt(depth, wu_v[...]).astype(BF)

    for k in (1, 2, 3):
        @pl.when(inside(-k))
        def _():
            near_send(k).start()

    spread(cgr, CGR, me)

    dep_all[me] = dep_mine[me // rep]
    stk_all[me] = stk_mine[me // rep]

    def give(src, dst, k):
        return pltpu.make_async_copy(src, dst, out_sem.at[k])

    half = ((level_v[...].astype(F32) - 1.0) * 0.5).reshape(1, ch)
    inverse = 1.0 / half

    def coder(frame, count):
        columns = jnp.concatenate(
            [lat[pl.ds(frame + p, count)].reshape(count * cells, ch) for p in range(3)], axis=1
        )
        squashed = jnp.tanh(mm(columns, wc_v[...]))
        bounded = half * squashed
        sine, cosine = half_turn(bounded)
        codes = ((bounded - sine * cosine * (2.0 / two_pi)) * inverse).astype(BF)
        return codes, (2.0 * sine * sine) * (1.0 - squashed * squashed)

    wc_flip = jnp.concatenate([wc_v[pl.ds((2 - p) * ch, ch)] for p in range(3)], axis=1)

    @pl.when(me < n - 1)
    def _():
        send_n().wait_recv()

    ahead = aligned(past(vbuf, 2, we_v, (0, 1, 2)))

    relay(lat, LAT, 2)

    @pl.loop(1, n)
    def _(k):
        block_send(STK, stk_mine, stk_all, peer_of(k)).start()

    def moved(perm, x):
        high = x.astype(BF)
        rest = (x - high.astype(F32)).astype(BF)
        return mm(perm, high) + mm(perm, rest)

    slopes = [
        moved(perm_v[0], slope_of(x, s))
        for x, s in ((pre_enc, sig), (ahead, jax.nn.sigmoid(ahead)))
    ]

    all_blocks(BUDDY + LAT, lat, half_n).wait_recv()
    step = min(n, 16)
    total = n * cells

    @pl.loop(0, n // step)
    def _(k):
        at = k * step
        codes, factor = coder(at, step)
        cod[pl.ds(at, step)] = codes.reshape(step, cells, ch)
        fac[pl.ds(at, step)] = factor.reshape(step, cells, ch)

    code_w[...] = cod[me].reshape(code_w.shape)
    code_out_copy = give(code_w, code_out, 0)
    code_out_copy.start()
    codes_turned = cod[...].reshape(total, ch).T
    lat_turned[...] = lat[0 : n + 2].reshape((n + 2) * cells, ch).T

    all_blocks(DEP, dep_all, n - 1).wait_recv()

    up_part = mm(codes_turned, dep_all[...].reshape(total, wb)) * scale
    block_rows = up_mine.shape[1]
    up_mine[...] = up_part.astype(BF).reshape(up_mine.shape)
    up_rows = ch // n
    mine = lax.rem(me, rep)
    my_block = me // rep

    def up_target(k):
        return mine + rep * lax.rem(my_block + k, nb)

    direct = block_rows == up_rows
    blocks_in = up_out if direct else up_all

    def up_send(peer):
        return block(UPS, up_mine.at[peer * up_rows // block_rows], blocks_in.at[my_block], peer)

    @pl.loop(1, nb)
    def _(k):
        up_send(up_target(k)).start()

    own_copy = give(up_mine.at[me * up_rows // block_rows], blocks_in.at[my_block], 4)
    own_copy.start()

    def take_rows(buf, at, out):
        count = out.shape[0]
        if count % 8 == 0:
            out[...] = buf[pl.ds(pl.multiple_of(at, 8), count)]
        else:
            for k in range(count):
                out[pl.ds(k, 1)] = buf[pl.ds(at + k, 1)]

    for k in (1, 2, 3):
        @pl.when(inside(k))
        def _():
            near_send(k).wait_recv()

    near_grads = jnp.concatenate([cgr[me], *[near[k] for k in range(3)]], axis=0).astype(F32)
    ahead_grad = near_grads * fac[pl.ds(me, 4)].reshape(4 * cells, ch)
    later = jnp.concatenate(
        [ahead_grad[p * cells : (p + 2) * cells].astype(BF) for p in range(3)], axis=1
    )
    grad_lat = mm_nt(later, wc_flip).astype(BF)

    deep_grad = mm_nt(grad_lat, wd_v[...])
    deep_rows = [
        jnp.concatenate(
            [
                deep_grad[frame * cells : (frame + 1) * cells, b * ch : (b + 1) * ch]
                for b in range(8)
            ],
            axis=0,
        )
        for frame in range(2)
    ]
    back = perm_v[1]
    for frame in range(2):
        ebuf[2 * frame : 2 * frame + 2, 1 : rows + 1] = (
            mm(back, (deep_rows[frame] * slopes[frame]).astype(BF))
            .astype(BF)
            .reshape(2, rows, width, ch)
        )
    hidden_grad = moved(back, deep_rows[0])

    bck = future(ebuf, 0, we_v, (0, 1, 2))
    vg_w[...] = (hidden_grad + aligned(bck)).astype(BF).reshape(vg_w.shape)
    vg_copy = give(vg_w, vg_out, 1)
    vg_copy.start()
    relay(cgr, CGR, 0)
    all_blocks(BUDDY + CGR, cgr, half_n).wait_recv()
    pre[2 : n + 2] = (cgr[0:n].astype(F32) * fac[0:n]).astype(BF)
    long = (n + 2) * cells
    coarse_rows = coarse_w.shape[0]
    piece = math.gcd(coarse_rows, ch)
    if piece % 16 == 0:
        for k in range(coarse_rows // piece):
            at = me * coarse_rows + k * piece
            left = lat_turned[pl.ds(pl.multiple_of(lax.rem(at, ch), piece), piece)]
            right = pre[pl.ds(2 - at // ch, n + 2)].reshape(long, ch)
            coarse_w[k * piece : (k + 1) * piece] = mm(left, right) * scale
    else:
        for p in range(3):
            coarse_v[pl.ds(p * ch, ch)] = (
                mm(lat_turned[...], pre[2 - p : 2 - p + n + 2].reshape(long, ch)) * scale
            )
        take_rows(coarse_v, me * coarse_rows, coarse_w)
    coarse_copy = give(coarse_w, coarse_out, 2)
    coarse_copy.start()
    later_all = jnp.concatenate([pre[2 + p : 2 + p + n].reshape(total, ch) for p in range(3)], axis=1)
    lgr[...] = mm_nt(later_all, wc_flip).astype(BF).reshape(lgr.shape)

    all_blocks(STK, stk_all, n - 1).wait_recv()

    whole_v[...] = (
        mm_tn(stk_all[...].reshape(total, wb), lgr[...].reshape(total, ch)) * scale
    )
    take_rows(whole_v, mine * down_out.shape[0], down_w)
    down_copy = give(down_w, down_out, 3)
    down_copy.start()

    @pl.when(me < n - 1)
    def _():
        send_v().wait_send()

    @pl.when(me > 0)
    def _():
        send_c().wait_send()
        send_n().wait_send()

    all_blocks(LAT, lat, half_n - 1).wait_send()
    all_blocks(CGR, cgr, half_n - 1).wait_send()
    all_blocks(BUDDY + LAT, lat, half_n).wait_send()
    all_blocks(BUDDY + CGR, cgr, half_n).wait_send()
    for k in (1, 2, 3):
        @pl.when(inside(-k))
        def _():
            near_send(k).wait_send()

    all_blocks(DEP, dep_all, n - 1).wait_send()
    all_blocks(STK, stk_all, n - 1).wait_send()
    for copy in (code_out_copy, vg_copy, coarse_copy, down_copy, own_copy):
        copy.wait()
    all_blocks(UPS, blocks_in, nb - 1).wait_recv()
    all_blocks(UPS, blocks_in, nb - 1).wait_send()
    if not direct:
        up_wide[...] = up_all[...].astype(F32)
        for b in range(nb):
            take_rows(up_wide.at[b], lax.rem(me * up_rows, block_rows), up_w.at[b])
        up_copy = give(up_w, up_out, 0)
        up_copy.start()
        up_copy.wait()


def tail(vg, code, down, coarse, up, vg_out, code_out, down_out, coarse_out, up_out, wide, sems):
    nb, _, wb = up.shape
    pairs = ((vg, vg_out), (code, code_out), (down, down_out), (coarse, coarse_out), (wide, up_out))
    copies = [pltpu.make_async_copy(src, dst, sems.at[k]) for k, (src, dst) in enumerate(pairs)]
    for copy in copies[:4]:
        copy.start()
    for b in range(nb):
        wide[:, b * wb : (b + 1) * wb] = up[b].astype(F32)
    copies[4].start()
    for copy in copies:
        copy.wait()


def shards(n, vf, ct, we, wd, wc, wu, wx, levels):
    frames, rows, width, ch = vf.shape
    deep = wd.shape[0]
    fine = frames * rows * width
    cells = fine // 8
    wb = max(128, deep // n)
    nb = deep // wb
    up_rows = ch // n
    block_rows = max(8, up_rows)
    scale = 1.0 / math.sqrt(n * fine)
    picks = depth_permutation(rows, width)
    perm = jnp.asarray(np.stack([picks, picks.T]), BF)
    anywhere = pl.BlockSpec(memory_space=pl.ANY)
    results = (
        (vf.shape, BF),
        ((frames // 2, rows // 2, width // 2, ch), BF),
        ((deep // n, ch), F32),
        ((wc.shape[0] // n, ch), F32),
        ((up_rows, deep), F32),
    )
    four = (4, rows + 2, width, ch)
    held_shapes = (
        results[0],
        results[1],
        results[2],
        results[3],
        ((nb, up_rows, wb), BF if block_rows == up_rows else F32),
    )
    scratch = [
        pltpu.VMEM(vf.shape, BF), pltpu.VMEM(results[1][0], BF), pltpu.VMEM(results[2][0], F32), pltpu.VMEM(results[3][0], F32),
        pltpu.VMEM((nb, up_rows, wb), F32), pltpu.VMEM((ch, (n + 2) * cells), BF),
        pltpu.VMEM((6, rows + 2, width, ch), BF), pltpu.VMEM(four, BF), pltpu.VMEM(four, BF),
        pltpu.VMEM(we.shape, BF), pltpu.VMEM(wx.shape, BF), pltpu.VMEM(wd.shape, BF),
        pltpu.VMEM(wc.shape, BF), pltpu.VMEM(wu.shape, BF), pltpu.VMEM(perm.shape, BF),
        pltpu.VMEM(levels.shape, jnp.int32),
        pltpu.VMEM((n + 5, cells, ch), BF), pltpu.VMEM((n, cells, ch), BF), pltpu.VMEM((3, cells, ch), BF),
        pltpu.VMEM((n, cells, ch), BF), pltpu.VMEM((n + 3, cells, ch), F32),
        pltpu.VMEM((n + 4, cells, ch), BF), pltpu.VMEM((n, cells, ch), BF),
        pltpu.VMEM((nb, cells, wb), BF), pltpu.VMEM((n, cells, wb), BF),
        pltpu.VMEM((nb, cells, wb), BF), pltpu.VMEM((n, cells, wb), BF),
        pltpu.VMEM((ch // block_rows, block_rows, wb), BF),
        pltpu.VMEM((nb, block_rows, wb), BF), pltpu.VMEM((nb, block_rows, wb), F32),
        pltpu.VMEM(wc.shape, F32), pltpu.VMEM((wb, ch), F32),
        pltpu.VMEM((3, fine, ch), F32), pltpu.VMEM((3, fine, ch), F32),
        pltpu.SemaphoreType.DMA((3,)), pltpu.SemaphoreType.DMA((3,)),
        pltpu.SemaphoreType.DMA((2, n // 2)), pltpu.SemaphoreType.DMA((3,)),
        pltpu.SemaphoreType.DMA((3,)), pltpu.SemaphoreType.DMA((7,)),
        pltpu.SemaphoreType.DMA((7,)), pltpu.SemaphoreType.DMA((11,)),
        pltpu.SemaphoreType.DMA((5,)),
        pltpu.SemaphoreType.REGULAR((n.bit_length() - 1,)),
    ]
    held = pl.pallas_call(
        functools.partial(kernel, n, scale),
        out_shape=tuple(pltpu.VMEM(*shape) for shape in held_shapes),
        in_specs=[anywhere] * 9,
        out_specs=(anywhere,) * 5,
        scratch_shapes=scratch,
        compiler_params=pltpu.CompilerParams(collective_id=0, has_side_effects=True),
    )(vf, ct, we, wd, wc, wu, wx, levels, perm)
    return pl.pallas_call(
        tail,
        out_shape=tuple(jax.ShapeDtypeStruct(*result) for result in results),
        in_specs=[anywhere] * 4 + [pl.BlockSpec(memory_space=pltpu.VMEM)],
        out_specs=(anywhere,) * 5,
        scratch_shapes=[pltpu.VMEM((up_rows, deep), F32), pltpu.SemaphoreType.DMA((5,))],
    )(*[pltpu.with_memory_space_constraint(part, pltpu.VMEM) for part in held])


def solution(mesh):
    placed = (P("tm", "grp", None, None), P("tm", "grp", None, None), P(), P(), P(), P(), P(), P())
    return jax.shard_map(
        functools.partial(shards, mesh.shape["tm"]),
        mesh=mesh,
        in_specs=placed,
        out_specs=(
            P("tm", "grp", None, None),
            P("tm", "grp", None, None),
            P(("grp", "tm"), None),
            P(("grp", "tm"), None),
            P(("grp", "tm"), None),
        ),
        check_vma=False,
    )
```

```python
import functools
import math

import jax
import jax.numpy as jnp
import numpy as np
from jax import lax
from jax.experimental import pallas as pl
from jax.experimental.pallas import tpu as pltpu
from jax.sharding import PartitionSpec as P

two_pi = 2.0 * math.pi
BF = jnp.bfloat16
F32 = jnp.float32
MESH = pl.DeviceIdType.MESH

HALO_V, HALO_C, HALO_N, HALO_W = 0, 1, 2, 3
LAT, CGR = 0, 1
BUDDY = 2
STK, DEP, UPS = 4, 5, 6

SINE = [(-1.0) ** k / math.factorial(2 * k + 1) for k in range(7)]
COSINE = [(-1.0) ** k / math.factorial(2 * k) for k in range(7)]

def mm(a, b):
    return jnp.dot(a, b, preferred_element_type=F32)


def mm_nt(a, b):
    return lax.dot_general(a, b, (((1,), (1,)), ((), ())), preferred_element_type=F32)


def mm_tn(a, b):
    return lax.dot_general(a, b, (((0,), (0,)), ((), ())), preferred_element_type=F32)


def half_turn(x):
    angle = (x - jnp.round(x)) * math.pi
    square = angle * angle
    sine, cosine = SINE[-1], COSINE[-1]
    for a, b in zip(SINE[-2::-1], COSINE[-2::-1]):
        sine = sine * square + a
        cosine = cosine * square + b
    return sine * angle, cosine


def depth_permutation(rows, cols):
    order = np.arange(2 * rows * cols).reshape(2, rows // 2, 2, cols // 2, 2)
    order = order.transpose(0, 2, 4, 1, 3).reshape(-1)
    picks = np.zeros((order.size, order.size), np.float32)
    picks[np.arange(order.size), order] = 1.0
    return picks


def kernel(
    n, scale, vf, ct, we, wd, wc, wu, wx, levels, perm,
    vg_out, code_out, down_out, coarse_out, up_out,
    vg_w, code_w, down_w, coarse_w, up_w, lat_turned,
    vbuf, cbuf, ebuf, we_v, wx_v, wd_v, wc_v, wu_v, perm_v, level_v,
    lat, cgr, near, cod, fac, pre, lgr, stk_mine, stk_all, dep_mine, dep_all, up_mine, up_all, up_wide, coarse_v, whole_v,
    acc_e, acc_d, hal_s, hal_r, msg_r, near_s, near_r, all_s, all_r, load_sem, out_sem, met,
):
    frames, rows, width, ch = vf.shape
    fine = frames * rows * width
    cells = fine // 8
    nb, _, wb = stk_mine.shape
    rep = n // nb
    me = lax.axis_index("tm")

    def peer_of(k):
        return lax.rem(me + k, n)

    odd = lax.rem(me, 2)
    buddy = me + 1 - 2 * odd
    other = me - 1 + 2 * odd
    has_other = (other >= 0) & (other < n)
    dims = n.bit_length() - 1

    def partner(d):
        return me + (1 - 2 * lax.rem(me // 2**d, 2)) * 2**d

    barrier = pltpu.get_barrier_semaphore()
    for d in range(dims):
        pl.semaphore_signal(barrier, inc=1, device_id={"tm": partner(d)}, device_id_type=MESH)

    @pl.when(has_other)
    def _():
        pl.semaphore_signal(barrier, inc=1, device_id={"tm": other}, device_id_type=MESH)

    def tell(d):
        if d < dims:
            pl.semaphore_signal(
                met.at[d], inc=1, device_id={"tm": partner(d)}, device_id_type=MESH
            )

    def hear(d):
        if d < dims:
            pl.semaphore_wait(met.at[d], 1)

    inner = pl.ds(1, rows)
    third = we.shape[0] // 3
    loads = [
        pltpu.make_async_copy(vf, vbuf.at[2:4, inner], load_sem.at[0]),
        pltpu.make_async_copy(ct, cbuf.at[0:2, inner], load_sem.at[1]),
    ]
    for k, (at, count) in enumerate(((2 * third, third), (0, 2 * third))):
        span = pl.ds(at, count)
        loads.append(pltpu.make_async_copy(we.at[span], we_v.at[span], load_sem.at[2 + 2 * k]))
        loads.append(pltpu.make_async_copy(wx.at[span], wx_v.at[span], load_sem.at[3 + 2 * k]))
    small = [
        pltpu.make_async_copy(src, dst, load_sem.at[6 + k])
        for k, (src, dst) in enumerate(
            ((perm, perm_v), (wd, wd_v), (wu, wu_v), (wc, wc_v), (levels, level_v))
        )
    ]
    for load in loads + small:
        load.start()

    def halo(kind, src, dst, peer):
        return pltpu.make_async_remote_copy(
            src_ref=src, dst_ref=dst, send_sem=hal_s.at[kind], recv_sem=hal_r.at[kind],
            device_id={"tm": peer}, device_id_type=MESH,
        )

    def block(kind, src, dst, peer, receives=None, sends=None):
        return pltpu.make_async_remote_copy(
            src_ref=src, dst_ref=dst,
            send_sem=all_s.at[kind] if sends is None else sends,
            recv_sem=all_r.at[kind] if receives is None else receives,
            device_id={"tm": peer}, device_id_type=MESH,
        )

    def all_blocks(kind, buf, count):
        return block(kind, buf.at[pl.ds(0, count)], buf.at[pl.ds(0, count)], buddy)

    def send_v():
        return halo(HALO_V, vbuf.at[3:4, inner], vbuf.at[1:2, inner], me + 1)

    def send_w():
        return halo(HALO_W, vbuf.at[2:3, inner], vbuf.at[0:1, inner], me + 1)

    def send_c():
        return halo(HALO_C, ct, cbuf.at[2:4, inner], me - 1)

    def send_n():
        return halo(HALO_N, vf, vbuf.at[4:6, inner], me - 1)

    for buf in (vbuf, cbuf, ebuf):
        edge = jnp.zeros((buf.shape[0], 1, width, ch), BF)
        buf[:, 0:1] = edge
        buf[:, rows + 1 : rows + 2] = edge
    blank = jnp.zeros((2, rows, width, ch), BF)

    @pl.when(me == 0)
    def _():
        vbuf[0:2, 1 : rows + 1] = blank

    @pl.when(me == n - 1)
    def _():
        cbuf[2:4, 1 : rows + 1] = blank
        vbuf[4:6, 1 : rows + 1] = blank

    lat[0:2] = jnp.zeros((2, cells, ch), BF)
    lat[n + 2 : n + 5] = jnp.zeros((3, cells, ch), BF)
    for k in (1, 2, 3):
        @pl.when(me + k >= n)
        def _():
            near[k - 1] = jnp.zeros((cells, ch), BF)

    fac[n : n + 3] = jnp.zeros((3, cells, ch), F32)
    pre[0:2] = jnp.zeros((2, cells, ch), BF)
    pre[n + 2 : n + 4] = jnp.zeros((2, cells, ch), BF)

    pl.semaphore_wait(barrier, jnp.where(has_other, dims + 1, dims))
    tell(0)

    loads[0].wait()

    @pl.when(me < n - 1)
    def _():
        send_v().start()
        send_w().start()

    @pl.when(me > 0)
    def _():
        send_c().start()
        send_n().start()

    def taps(buf, at):
        return jnp.concatenate(
            [buf[at : at + 2, q : q + rows].reshape(fine, ch) for q in range(3)], axis=1
        )

    def past(buf, at, weight, parts):
        left = jnp.concatenate([taps(buf, at + p) for p in parts], axis=1)
        out = []
        for r in range(3):
            right = jnp.concatenate(
                [
                    weight[pl.ds(((3 * p + q) * 3 + r) * ch, ch)]
                    for p in parts
                    for q in range(3)
                ],
                axis=0,
            )
            out.append(mm(left, right))
        return out

    def future(buf, at, weight, parts):
        left = jnp.concatenate([taps(buf, at + p) for p in parts], axis=1)
        out = []
        for r in range(3):
            right = jnp.concatenate(
                [
                    weight[pl.ds((((2 - p) * 3 + 2 - q) * 3 + 2 - r) * ch, ch)]
                    for p in parts
                    for q in range(3)
                ],
                axis=1,
            )
            out.append(mm_nt(left, right))
        return out

    def keep(acc, parts):
        for r in range(3):
            acc[r] = parts[r]

    def added(acc, parts):
        return [acc[r] + parts[r] for r in range(3)]

    lane = lax.broadcasted_iota(jnp.int32, (fine // width, width, ch), 1)

    def aligned(parts):
        a, b, c = [x.reshape(fine // width, width, ch) for x in parts]
        a = jnp.where(lane == 0, 0.0, pltpu.roll(a, 1, 1))
        c = jnp.where(lane == width - 1, 0.0, pltpu.roll(c, width - 1, 1))
        return (a + b + c).reshape(fine, ch)

    hear(0)
    tell(1)

    loads[2].wait()
    keep(acc_e, past(vbuf, 0, we_v, (2,)))
    hear(1)
    tell(2)
    loads[1].wait()
    loads[3].wait()
    keep(acc_d, future(cbuf, 0, wx_v, (0,)))
    hear(2)
    tell(3)
    loads[4].wait()

    @pl.when(me > 0)
    def _():
        send_v().wait_recv()

    keep(acc_e, added(acc_e, past(vbuf, 0, we_v, (1,))))

    @pl.when(me > 0)
    def _():
        send_w().wait_recv()

    enc = added(acc_e, past(vbuf, 0, we_v, (0,)))
    pre_enc = aligned(enc)
    sig = jax.nn.sigmoid(pre_enc)
    own = vbuf[2:4, 1 : rows + 1].reshape(fine, ch).astype(F32)
    hidden = (own + pre_enc * sig).astype(BF)

    def slope_of(x, s):
        return s * (1.0 + x * (1.0 - s))

    for load in small:
        load.wait()

    def regroup(field, store):
        moved = mm(perm_v[0], field)
        blocks = [moved[b * cells : (b + 1) * cells].astype(BF) for b in range(8)]
        per = nb // 8
        for b in range(8):
            for h in range(per):
                store[b * per + h] = blocks[b][:, h * wb : (h + 1) * wb]
        return jnp.concatenate(blocks, axis=1)

    half_n = n // 2

    def parity_send(buf, kind, slot, k):
        peer = lax.rem(me + 2 * k, n)
        return block(kind, buf.at[slot], buf.at[slot], peer, msg_r.at[kind, me // 2])

    def buddy_send(buf, kind, slot):
        return block(BUDDY + kind, buf.at[slot], buf.at[slot], buddy)

    def near_send(k):
        return block(
            CGR, cgr.at[me], near.at[k - 1], me - k, near_r.at[k - 1], near_s.at[k - 1]
        )

    def arrival(buf, kind, slot, source):
        return block(kind, buf.at[slot], buf.at[slot], buddy, msg_r.at[kind, source // 2])

    def inside(k):
        return (me + k >= 0) & (me + k < n)

    def spread(buf, kind, slot):
        buddy_send(buf, kind, slot).start()

        @pl.loop(1, half_n)
        def _(k):
            parity_send(buf, kind, slot, k).start()

    def relay(buf, kind, shift):
        @pl.loop(1, half_n)
        def _(k):
            source = lax.rem(me + n - 2 * k, n)
            slot = source + shift
            arrival(buf, kind, slot, source).wait_recv()
            block(BUDDY + kind, buf.at[slot], buf.at[slot], buddy).start()

    lat[me + 2] = mm(regroup(hidden, stk_mine), wd_v[...]).astype(BF)
    hear(3)
    for d in range(4, dims):
        tell(d)
        hear(d)
    spread(lat, LAT, me + 2)

    loads[5].wait()

    @pl.when(me < n - 1)
    def _():
        send_c().wait_recv()

    dec = added(acc_d, future(cbuf, 0, wx_v, (1, 2)))
    own_c = cbuf[0:2, 1 : rows + 1].reshape(fine, ch).astype(F32)
    depth = regroup((own_c + aligned(dec)).astype(BF), dep_mine)

    def block_send(kind, mine, everyone, peer):
        return block(kind, mine.at[peer // rep], everyone.at[me], peer)

    @pl.loop(1, n)
    def _(k):
        block_send(DEP, dep_mine, dep_all, peer_of(k)).start()

    cgr[me] = mm_nt(depth, wu_v[...]).astype(BF)

    for k in (1, 2, 3):
        @pl.when(inside(-k))
        def _():
            near_send(k).start()

    spread(cgr, CGR, me)

    dep_all[me] = dep_mine[me // rep]
    stk_all[me] = stk_mine[me // rep]

    def give(src, dst, k):
        return pltpu.make_async_copy(src, dst, out_sem.at[k])

    half = ((level_v[...].astype(F32) - 1.0) * 0.5).reshape(1, ch)
    inverse = 1.0 / half

    def coder(frame, count):
        columns = jnp.concatenate(
            [lat[pl.ds(frame + p, count)].reshape(count * cells, ch) for p in range(3)], axis=1
        )
        squashed = jnp.tanh(mm(columns, wc_v[...]))
        bounded = half * squashed
        sine, cosine = half_turn(bounded)
        codes = ((bounded - sine * cosine * (2.0 / two_pi)) * inverse).astype(BF)
        return codes, (2.0 * sine * sine) * (1.0 - squashed * squashed)

    wc_flip = jnp.concatenate([wc_v[pl.ds((2 - p) * ch, ch)] for p in range(3)], axis=1)

    @pl.when(me < n - 1)
    def _():
        send_n().wait_recv()

    ahead = aligned(past(vbuf, 2, we_v, (0, 1, 2)))

    relay(lat, LAT, 2)

    @pl.loop(1, n)
    def _(k):
        block_send(STK, stk_mine, stk_all, peer_of(k)).start()

    def moved(perm, x):
        high = x.astype(BF)
        rest = (x - high.astype(F32)).astype(BF)
        return mm(perm, high) + mm(perm, rest)

    slopes = [
        moved(perm_v[0], slope_of(x, s))
        for x, s in ((pre_enc, sig), (ahead, jax.nn.sigmoid(ahead)))
    ]

    all_blocks(BUDDY + LAT, lat, half_n).wait_recv()
    step = min(n, 16)
    total = n * cells

    @pl.loop(0, n // step)
    def _(k):
        at = k * step
        codes, factor = coder(at, step)
        cod[pl.ds(at, step)] = codes.reshape(step, cells, ch)
        fac[pl.ds(at, step)] = factor.reshape(step, cells, ch)

    code_w[...] = cod[me].reshape(code_w.shape)
    code_out_copy = give(code_w, code_out, 0)
    code_out_copy.start()
    codes_turned = cod[...].reshape(total, ch).T
    lat_turned[...] = lat[0 : n + 2].reshape((n + 2) * cells, ch).T

    all_blocks(DEP, dep_all, n - 1).wait_recv()

    up_part = mm(codes_turned, dep_all[...].reshape(total, wb)) * scale
    block_rows = up_mine.shape[1]
    up_mine[...] = up_part.astype(BF).reshape(up_mine.shape)
    up_rows = ch // n
    mine = lax.rem(me, rep)
    my_block = me // rep

    def up_target(k):
        return mine + rep * lax.rem(my_block + k, nb)

    direct = block_rows == up_rows
    blocks_in = up_out if direct else up_all

    def up_send(peer):
        return block(UPS, up_mine.at[peer * up_rows // block_rows], blocks_in.at[my_block], peer)

    @pl.loop(1, nb)
    def _(k):
        up_send(up_target(k)).start()

    own_copy = give(up_mine.at[me * up_rows // block_rows], blocks_in.at[my_block], 4)
    own_copy.start()

    def take_rows(buf, at, out):
        count = out.shape[0]
        if count % 8 == 0:
            out[...] = buf[pl.ds(pl.multiple_of(at, 8), count)]
        else:
            for k in range(count):
                out[pl.ds(k, 1)] = buf[pl.ds(at + k, 1)]

    for k in (1, 2, 3):
        @pl.when(inside(k))
        def _():
            near_send(k).wait_recv()

    near_grads = jnp.concatenate([cgr[me], *[near[k] for k in range(3)]], axis=0).astype(F32)
    ahead_grad = near_grads * fac[pl.ds(me, 4)].reshape(4 * cells, ch)
    later = jnp.concatenate(
        [ahead_grad[p * cells : (p + 2) * cells].astype(BF) for p in range(3)], axis=1
    )
    grad_lat = mm_nt(later, wc_flip).astype(BF)

    deep_grad = mm_nt(grad_lat, wd_v[...])
    deep_rows = [
        jnp.concatenate(
            [
                deep_grad[frame * cells : (frame + 1) * cells, b * ch : (b + 1) * ch]
                for b in range(8)
            ],
            axis=0,
        )
        for frame in range(2)
    ]
    back = perm_v[1]
    for frame in range(2):
        ebuf[2 * frame : 2 * frame + 2, 1 : rows + 1] = (
            mm(back, (deep_rows[frame] * slopes[frame]).astype(BF))
            .astype(BF)
            .reshape(2, rows, width, ch)
        )
    hidden_grad = moved(back, deep_rows[0])

    bck = future(ebuf, 0, we_v, (0, 1, 2))
    vg_w[...] = (hidden_grad + aligned(bck)).astype(BF).reshape(vg_w.shape)
    vg_copy = give(vg_w, vg_out, 1)
    vg_copy.start()
    relay(cgr, CGR, 0)
    all_blocks(BUDDY + CGR, cgr, half_n).wait_recv()
    pre[2 : n + 2] = (cgr[0:n].astype(F32) * fac[0:n]).astype(BF)
    long = (n + 2) * cells
    coarse_rows = coarse_w.shape[0]
    piece = math.gcd(coarse_rows, ch)
    if piece % 16 == 0:
        for k in range(coarse_rows // piece):
            at = me * coarse_rows + k * piece
            left = lat_turned[pl.ds(pl.multiple_of(lax.rem(at, ch), piece), piece)]
            right = pre[pl.ds(2 - at // ch, n + 2)].reshape(long, ch)
            coarse_w[k * piece : (k + 1) * piece] = mm(left, right) * scale
    else:
        for p in range(3):
            coarse_v[pl.ds(p * ch, ch)] = (
                mm(lat_turned[...], pre[2 - p : 2 - p + n + 2].reshape(long, ch)) * scale
            )
        take_rows(coarse_v, me * coarse_rows, coarse_w)
    coarse_copy = give(coarse_w, coarse_out, 2)
    coarse_copy.start()
    later_all = jnp.concatenate([pre[2 + p : 2 + p + n].reshape(total, ch) for p in range(3)], axis=1)
    lgr[...] = mm_nt(later_all, wc_flip).astype(BF).reshape(lgr.shape)

    all_blocks(STK, stk_all, n - 1).wait_recv()

    whole_v[...] = (
        mm_tn(stk_all[...].reshape(total, wb), lgr[...].reshape(total, ch)) * scale
    )
    take_rows(whole_v, mine * down_out.shape[0], down_w)
    down_copy = give(down_w, down_out, 3)
    down_copy.start()

    @pl.when(me < n - 1)
    def _():
        send_v().wait_send()
        send_w().wait_send()

    @pl.when(me > 0)
    def _():
        send_c().wait_send()
        send_n().wait_send()

    all_blocks(LAT, lat, half_n - 1).wait_send()
    all_blocks(CGR, cgr, half_n - 1).wait_send()
    all_blocks(BUDDY + LAT, lat, half_n).wait_send()
    all_blocks(BUDDY + CGR, cgr, half_n).wait_send()
    for k in (1, 2, 3):
        @pl.when(inside(-k))
        def _():
            near_send(k).wait_send()

    all_blocks(DEP, dep_all, n - 1).wait_send()
    all_blocks(STK, stk_all, n - 1).wait_send()
    for copy in (code_out_copy, vg_copy, coarse_copy, down_copy, own_copy):
        copy.wait()
    all_blocks(UPS, blocks_in, nb - 1).wait_recv()
    all_blocks(UPS, blocks_in, nb - 1).wait_send()
    if not direct:
        up_wide[...] = up_all[...].astype(F32)
        for b in range(nb):
            take_rows(up_wide.at[b], lax.rem(me * up_rows, block_rows), up_w.at[b])
        up_copy = give(up_w, up_out, 0)
        up_copy.start()
        up_copy.wait()


def tail(vg, code, down, coarse, up, vg_out, code_out, down_out, coarse_out, up_out, wide, sems):
    nb, _, wb = up.shape
    pairs = ((vg, vg_out), (code, code_out), (down, down_out), (coarse, coarse_out), (wide, up_out))
    copies = [pltpu.make_async_copy(src, dst, sems.at[k]) for k, (src, dst) in enumerate(pairs)]
    for copy in copies[:4]:
        copy.start()
    for b in range(nb):
        wide[:, b * wb : (b + 1) * wb] = up[b].astype(F32)
    copies[4].start()
    for copy in copies:
        copy.wait()


def shards(n, vf, ct, we, wd, wc, wu, wx, levels):
    frames, rows, width, ch = vf.shape
    deep = wd.shape[0]
    fine = frames * rows * width
    cells = fine // 8
    wb = max(128, deep // n)
    nb = deep // wb
    up_rows = ch // n
    block_rows = max(8, up_rows)
    scale = 1.0 / math.sqrt(n * fine)
    picks = depth_permutation(rows, width)
    perm = jnp.asarray(np.stack([picks, picks.T]), BF)
    anywhere = pl.BlockSpec(memory_space=pl.ANY)
    results = (
        (vf.shape, BF),
        ((frames // 2, rows // 2, width // 2, ch), BF),
        ((deep // n, ch), F32),
        ((wc.shape[0] // n, ch), F32),
        ((up_rows, deep), F32),
    )
    four = (4, rows + 2, width, ch)
    held_shapes = (
        results[0],
        results[1],
        results[2],
        results[3],
        ((nb, up_rows, wb), BF if block_rows == up_rows else F32),
    )
    scratch = [
        pltpu.VMEM(vf.shape, BF), pltpu.VMEM(results[1][0], BF), pltpu.VMEM(results[2][0], F32), pltpu.VMEM(results[3][0], F32),
        pltpu.VMEM((nb, up_rows, wb), F32), pltpu.VMEM((ch, (n + 2) * cells), BF),
        pltpu.VMEM((6, rows + 2, width, ch), BF), pltpu.VMEM(four, BF), pltpu.VMEM(four, BF),
        pltpu.VMEM(we.shape, BF), pltpu.VMEM(wx.shape, BF), pltpu.VMEM(wd.shape, BF),
        pltpu.VMEM(wc.shape, BF), pltpu.VMEM(wu.shape, BF), pltpu.VMEM(perm.shape, BF),
        pltpu.VMEM(levels.shape, jnp.int32),
        pltpu.VMEM((n + 5, cells, ch), BF), pltpu.VMEM((n, cells, ch), BF), pltpu.VMEM((3, cells, ch), BF),
        pltpu.VMEM((n, cells, ch), BF), pltpu.VMEM((n + 3, cells, ch), F32),
        pltpu.VMEM((n + 4, cells, ch), BF), pltpu.VMEM((n, cells, ch), BF),
        pltpu.VMEM((nb, cells, wb), BF), pltpu.VMEM((n, cells, wb), BF),
        pltpu.VMEM((nb, cells, wb), BF), pltpu.VMEM((n, cells, wb), BF),
        pltpu.VMEM((ch // block_rows, block_rows, wb), BF),
        pltpu.VMEM((nb, block_rows, wb), BF), pltpu.VMEM((nb, block_rows, wb), F32),
        pltpu.VMEM(wc.shape, F32), pltpu.VMEM((wb, ch), F32),
        pltpu.VMEM((3, fine, ch), F32), pltpu.VMEM((3, fine, ch), F32),
        pltpu.SemaphoreType.DMA((4,)), pltpu.SemaphoreType.DMA((4,)),
        pltpu.SemaphoreType.DMA((2, n // 2)), pltpu.SemaphoreType.DMA((3,)),
        pltpu.SemaphoreType.DMA((3,)), pltpu.SemaphoreType.DMA((7,)),
        pltpu.SemaphoreType.DMA((7,)), pltpu.SemaphoreType.DMA((11,)),
        pltpu.SemaphoreType.DMA((5,)),
        pltpu.SemaphoreType.REGULAR((n.bit_length() - 1,)),
    ]
    held = pl.pallas_call(
        functools.partial(kernel, n, scale),
        out_shape=tuple(pltpu.VMEM(*shape) for shape in held_shapes),
        in_specs=[anywhere] * 9,
        out_specs=(anywhere,) * 5,
        scratch_shapes=scratch,
        compiler_params=pltpu.CompilerParams(collective_id=0, has_side_effects=True),
    )(vf, ct, we, wd, wc, wu, wx, levels, perm)
    return pl.pallas_call(
        tail,
        out_shape=tuple(jax.ShapeDtypeStruct(*result) for result in results),
        in_specs=[anywhere] * 4 + [pl.BlockSpec(memory_space=pltpu.VMEM)],
        out_specs=(anywhere,) * 5,
        scratch_shapes=[pltpu.VMEM((up_rows, deep), F32), pltpu.SemaphoreType.DMA((5,))],
    )(*[pltpu.with_memory_space_constraint(part, pltpu.VMEM) for part in held])


def solution(mesh):
    placed = (P("tm", "grp", None, None), P("tm", "grp", None, None), P(), P(), P(), P(), P(), P())
    return jax.shard_map(
        functools.partial(shards, mesh.shape["tm"]),
        mesh=mesh,
        in_specs=placed,
        out_specs=(
            P("tm", "grp", None, None),
            P("tm", "grp", None, None),
            P(("grp", "tm"), None),
            P(("grp", "tm"), None),
            P(("grp", "tm"), None),
        ),
        check_vma=False,
    )
```

```python
import functools
import math

import jax
import jax.numpy as jnp
import numpy as np
from jax import lax
from jax.experimental import pallas as pl
from jax.experimental.pallas import tpu as pltpu
from jax.sharding import PartitionSpec as P

two_pi = 2.0 * math.pi
BF = jnp.bfloat16
F32 = jnp.float32
MESH = pl.DeviceIdType.MESH

HALO_V, HALO_C, HALO_N, HALO_W = 0, 1, 2, 3
LAT, CGR = 0, 1
BUDDY = 2
STK, DEP, UPS = 4, 5, 6

SINE = [(-1.0) ** k / math.factorial(2 * k + 1) for k in range(7)]
COSINE = [(-1.0) ** k / math.factorial(2 * k) for k in range(7)]

def mm(a, b):
    return jnp.dot(a, b, preferred_element_type=F32)


def mm_nt(a, b):
    return lax.dot_general(a, b, (((1,), (1,)), ((), ())), preferred_element_type=F32)


def mm_tn(a, b):
    return lax.dot_general(a, b, (((0,), (0,)), ((), ())), preferred_element_type=F32)


def half_turn(x):
    angle = (x - jnp.round(x)) * math.pi
    square = angle * angle
    sine, cosine = SINE[-1], COSINE[-1]
    for a, b in zip(SINE[-2::-1], COSINE[-2::-1]):
        sine = sine * square + a
        cosine = cosine * square + b
    return sine * angle, cosine


def depth_permutation(rows, cols):
    order = np.arange(2 * rows * cols).reshape(2, rows // 2, 2, cols // 2, 2)
    order = order.transpose(0, 2, 4, 1, 3).reshape(-1)
    picks = np.zeros((order.size, order.size), np.float32)
    picks[np.arange(order.size), order] = 1.0
    return picks


def kernel(
    n, scale, vf, ct, we, wd, wc, wu, wx, levels, perm,
    vg_out, code_out, down_out, coarse_out, up_out,
    vg_w, code_w, down_w, coarse_w, up_w, lat_turned, wd_t, wc_t,
    vbuf, cbuf, ebuf, we_v, wx_v, wd_v, wc_v, wu_v, perm_v, level_v,
    lat, cgr, near, cod, fac, pre, lgr, stk_mine, stk_all, dep_mine, dep_all, up_mine, up_all, up_wide, coarse_v, whole_v,
    acc_e, acc_d, hal_s, hal_r, msg_r, near_s, near_r, all_s, all_r, load_sem, out_sem, met,
):
    frames, rows, width, ch = vf.shape
    fine = frames * rows * width
    cells = fine // 8
    nb, _, wb = stk_mine.shape
    rep = n // nb
    me = lax.axis_index("tm")

    def peer_of(k):
        return lax.rem(me + k, n)

    odd = lax.rem(me, 2)
    buddy = me + 1 - 2 * odd
    other = me - 1 + 2 * odd
    has_other = (other >= 0) & (other < n)
    dims = n.bit_length() - 1

    def partner(d):
        return me + (1 - 2 * lax.rem(me // 2**d, 2)) * 2**d

    barrier = pltpu.get_barrier_semaphore()
    for d in range(dims):
        pl.semaphore_signal(barrier, inc=1, device_id={"tm": partner(d)}, device_id_type=MESH)

    @pl.when(has_other)
    def _():
        pl.semaphore_signal(barrier, inc=1, device_id={"tm": other}, device_id_type=MESH)

    def tell(d):
        if d < dims:
            pl.semaphore_signal(
                met.at[d], inc=1, device_id={"tm": partner(d)}, device_id_type=MESH
            )

    def hear(d):
        if d < dims:
            pl.semaphore_wait(met.at[d], 1)

    inner = pl.ds(1, rows)
    third = we.shape[0] // 3
    loads = [
        pltpu.make_async_copy(vf, vbuf.at[2:4, inner], load_sem.at[0]),
        pltpu.make_async_copy(ct, cbuf.at[0:2, inner], load_sem.at[1]),
    ]
    for k, (at, count) in enumerate(((2 * third, third), (0, 2 * third))):
        span = pl.ds(at, count)
        loads.append(pltpu.make_async_copy(we.at[span], we_v.at[span], load_sem.at[2 + 2 * k]))
        loads.append(pltpu.make_async_copy(wx.at[span], wx_v.at[span], load_sem.at[3 + 2 * k]))
    small = [
        pltpu.make_async_copy(src, dst, load_sem.at[6 + k])
        for k, (src, dst) in enumerate(
            ((perm, perm_v), (wd, wd_v), (wu, wu_v), (wc, wc_v), (levels, level_v))
        )
    ]
    for load in loads + small:
        load.start()

    def halo(kind, src, dst, peer):
        return pltpu.make_async_remote_copy(
            src_ref=src, dst_ref=dst, send_sem=hal_s.at[kind], recv_sem=hal_r.at[kind],
            device_id={"tm": peer}, device_id_type=MESH,
        )

    def block(kind, src, dst, peer, receives=None, sends=None):
        return pltpu.make_async_remote_copy(
            src_ref=src, dst_ref=dst,
            send_sem=all_s.at[kind] if sends is None else sends,
            recv_sem=all_r.at[kind] if receives is None else receives,
            device_id={"tm": peer}, device_id_type=MESH,
        )

    def all_blocks(kind, buf, count):
        return block(kind, buf.at[pl.ds(0, count)], buf.at[pl.ds(0, count)], buddy)

    def send_v():
        return halo(HALO_V, vbuf.at[3:4, inner], vbuf.at[1:2, inner], me + 1)

    def send_w():
        return halo(HALO_W, vbuf.at[2:3, inner], vbuf.at[0:1, inner], me + 1)

    def send_c():
        return halo(HALO_C, ct, cbuf.at[2:4, inner], me - 1)

    def send_n():
        return halo(HALO_N, vf, vbuf.at[4:6, inner], me - 1)

    for buf in (vbuf, cbuf, ebuf):
        edge = jnp.zeros((buf.shape[0], 1, width, ch), BF)
        buf[:, 0:1] = edge
        buf[:, rows + 1 : rows + 2] = edge
    blank = jnp.zeros((2, rows, width, ch), BF)

    @pl.when(me == 0)
    def _():
        vbuf[0:2, 1 : rows + 1] = blank

    @pl.when(me == n - 1)
    def _():
        cbuf[2:4, 1 : rows + 1] = blank
        vbuf[4:6, 1 : rows + 1] = blank

    lat[0:2] = jnp.zeros((2, cells, ch), BF)
    lat[n + 2 : n + 5] = jnp.zeros((3, cells, ch), BF)
    for k in (1, 2, 3):
        @pl.when(me + k >= n)
        def _():
            near[k - 1] = jnp.zeros((cells, ch), BF)

    fac[n : n + 3] = jnp.zeros((3, cells, ch), F32)
    pre[0:2] = jnp.zeros((2, cells, ch), BF)
    pre[n + 2 : n + 4] = jnp.zeros((2, cells, ch), BF)

    pl.semaphore_wait(barrier, jnp.where(has_other, dims + 1, dims))
    tell(0)

    loads[0].wait()

    @pl.when(me < n - 1)
    def _():
        send_v().start()
        send_w().start()

    @pl.when(me > 0)
    def _():
        send_c().start()
        send_n().start()

    def taps(buf, at):
        return jnp.concatenate(
            [buf[at : at + 2, q : q + rows].reshape(fine, ch) for q in range(3)], axis=1
        )

    def past(buf, at, weight, parts):
        left = jnp.concatenate([taps(buf, at + p) for p in parts], axis=1)
        out = []
        for r in range(3):
            right = jnp.concatenate(
                [
                    weight[pl.ds(((3 * p + q) * 3 + r) * ch, ch)]
                    for p in parts
                    for q in range(3)
                ],
                axis=0,
            )
            out.append(mm(left, right))
        return out

    def future(buf, at, weight, parts):
        left = jnp.concatenate([taps(buf, at + p) for p in parts], axis=1)
        out = []
        for r in range(3):
            right = jnp.concatenate(
                [
                    weight[pl.ds((((2 - p) * 3 + 2 - q) * 3 + 2 - r) * ch, ch)]
                    for p in parts
                    for q in range(3)
                ],
                axis=1,
            )
            out.append(mm_nt(left, right))
        return out

    def keep(acc, parts):
        for r in range(3):
            acc[r] = parts[r]

    def added(acc, parts):
        return [acc[r] + parts[r] for r in range(3)]

    lane = lax.broadcasted_iota(jnp.int32, (fine // width, width, ch), 1)

    def aligned(parts):
        a, b, c = [x.reshape(fine // width, width, ch) for x in parts]
        a = jnp.where(lane == 0, 0.0, pltpu.roll(a, 1, 1))
        c = jnp.where(lane == width - 1, 0.0, pltpu.roll(c, width - 1, 1))
        return (a + b + c).reshape(fine, ch)

    hear(0)
    tell(1)

    loads[2].wait()
    hear(1)
    tell(2)
    keep(acc_e, past(vbuf, 0, we_v, (2,)))
    hear(2)
    tell(3)
    loads[1].wait()
    loads[3].wait()
    keep(acc_d, future(cbuf, 0, wx_v, (0,)))
    loads[4].wait()

    @pl.when(me > 0)
    def _():
        send_v().wait_recv()

    keep(acc_e, added(acc_e, past(vbuf, 0, we_v, (1,))))

    @pl.when(me > 0)
    def _():
        send_w().wait_recv()

    enc = added(acc_e, past(vbuf, 0, we_v, (0,)))
    pre_enc = aligned(enc)
    sig = jax.nn.sigmoid(pre_enc)
    own = vbuf[2:4, 1 : rows + 1].reshape(fine, ch).astype(F32)
    hidden = (own + pre_enc * sig).astype(BF)

    def slope_of(x, s):
        return s * (1.0 + x * (1.0 - s))

    for load in small:
        load.wait()

    def regroup(field, store):
        moved = mm(perm_v[0], field)
        blocks = [moved[b * cells : (b + 1) * cells].astype(BF) for b in range(8)]
        per = nb // 8
        for b in range(8):
            for h in range(per):
                store[b * per + h] = blocks[b][:, h * wb : (h + 1) * wb]
        return jnp.concatenate(blocks, axis=1)

    half_n = n // 2

    def parity_send(buf, kind, slot, k):
        peer = lax.rem(me + 2 * k, n)
        return block(kind, buf.at[slot], buf.at[slot], peer, msg_r.at[kind, me // 2])

    def buddy_send(buf, kind, slot):
        return block(BUDDY + kind, buf.at[slot], buf.at[slot], buddy)

    def near_send(k):
        return block(
            CGR, cgr.at[me], near.at[k - 1], me - k, near_r.at[k - 1], near_s.at[k - 1]
        )

    def arrival(buf, kind, slot, source):
        return block(kind, buf.at[slot], buf.at[slot], buddy, msg_r.at[kind, source // 2])

    def inside(k):
        return (me + k >= 0) & (me + k < n)

    def spread(buf, kind, slot):
        buddy_send(buf, kind, slot).start()

        @pl.loop(1, half_n)
        def _(k):
            parity_send(buf, kind, slot, k).start()

    def relay(buf, kind, shift):
        @pl.loop(1, half_n)
        def _(k):
            source = lax.rem(me + n - 2 * k, n)
            slot = source + shift
            arrival(buf, kind, slot, source).wait_recv()
            block(BUDDY + kind, buf.at[slot], buf.at[slot], buddy).start()

    lat[me + 2] = mm(regroup(hidden, stk_mine), wd_v[...]).astype(BF)
    hear(3)
    for d in range(4, dims):
        tell(d)
        hear(d)
    spread(lat, LAT, me + 2)

    loads[5].wait()

    @pl.when(me < n - 1)
    def _():
        send_c().wait_recv()

    dec = added(acc_d, future(cbuf, 0, wx_v, (1, 2)))
    own_c = cbuf[0:2, 1 : rows + 1].reshape(fine, ch).astype(F32)
    depth = regroup((own_c + aligned(dec)).astype(BF), dep_mine)

    def block_send(kind, mine, everyone, peer):
        return block(kind, mine.at[peer // rep], everyone.at[me], peer)

    @pl.loop(1, n)
    def _(k):
        block_send(DEP, dep_mine, dep_all, peer_of(k)).start()

    cgr[me] = mm_nt(depth, wu_v[...]).astype(BF)

    for k in (1, 2, 3):
        @pl.when(inside(-k))
        def _():
            near_send(k).start()

    spread(cgr, CGR, me)

    dep_all[me] = dep_mine[me // rep]
    stk_all[me] = stk_mine[me // rep]

    def give(src, dst, k):
        return pltpu.make_async_copy(src, dst, out_sem.at[k])

    half = ((level_v[...].astype(F32) - 1.0) * 0.5).reshape(1, ch)
    inverse = 1.0 / half

    def coder(frame, count):
        columns = jnp.concatenate(
            [lat[pl.ds(frame + p, count)].reshape(count * cells, ch) for p in range(3)], axis=1
        )
        squashed = jnp.tanh(mm(columns, wc_v[...]))
        bounded = half * squashed
        sine, cosine = half_turn(bounded)
        codes = ((bounded - sine * cosine * (2.0 / two_pi)) * inverse).astype(BF)
        return codes, (2.0 * sine * sine) * (1.0 - squashed * squashed)

    @pl.when(me < n - 1)
    def _():
        send_n().wait_recv()

    ahead = aligned(past(vbuf, 2, we_v, (0, 1, 2)))

    relay(lat, LAT, 2)

    @pl.loop(1, n)
    def _(k):
        block_send(STK, stk_mine, stk_all, peer_of(k)).start()

    def moved(perm, x):
        high = x.astype(BF)
        rest = (x - high.astype(F32)).astype(BF)
        return mm(perm, high) + mm(perm, rest)

    slopes = [
        moved(perm_v[0], slope_of(x, s))
        for x, s in ((pre_enc, sig), (ahead, jax.nn.sigmoid(ahead)))
    ]

    wd_t[...] = wd_v[...].T
    for p in range(3):
        wc_t[p * ch : (p + 1) * ch] = wc_v[(2 - p) * ch : (3 - p) * ch].T

    all_blocks(BUDDY + LAT, lat, half_n).wait_recv()
    step = min(n, 16)
    total = n * cells

    @pl.loop(0, n // step)
    def _(k):
        at = k * step
        codes, factor = coder(at, step)
        cod[pl.ds(at, step)] = codes.reshape(step, cells, ch)
        fac[pl.ds(at, step)] = factor.reshape(step, cells, ch)

    code_w[...] = cod[me].reshape(code_w.shape)
    code_out_copy = give(code_w, code_out, 0)
    code_out_copy.start()
    codes_turned = cod[...].reshape(total, ch).T
    lat_turned[...] = lat[0 : n + 2].reshape((n + 2) * cells, ch).T

    all_blocks(DEP, dep_all, n - 1).wait_recv()

    up_part = mm(codes_turned, dep_all[...].reshape(total, wb)) * scale
    block_rows = up_mine.shape[1]
    up_mine[...] = up_part.astype(BF).reshape(up_mine.shape)
    up_rows = ch // n
    mine = lax.rem(me, rep)
    my_block = me // rep

    def up_target(k):
        return mine + rep * lax.rem(my_block + k, nb)

    direct = block_rows == up_rows
    blocks_in = up_out if direct else up_all

    def up_send(peer):
        return block(UPS, up_mine.at[peer * up_rows // block_rows], blocks_in.at[my_block], peer)

    @pl.loop(1, nb)
    def _(k):
        up_send(up_target(k)).start()

    own_copy = give(up_mine.at[me * up_rows // block_rows], blocks_in.at[my_block], 4)
    own_copy.start()

    def take_rows(buf, at, out):
        count = out.shape[0]
        if count % 8 == 0:
            out[...] = buf[pl.ds(pl.multiple_of(at, 8), count)]
        else:
            for k in range(count):
                out[pl.ds(k, 1)] = buf[pl.ds(at + k, 1)]

    for k in (1, 2, 3):
        @pl.when(inside(k))
        def _():
            near_send(k).wait_recv()

    near_grads = jnp.concatenate([cgr[me], *[near[k] for k in range(3)]], axis=0).astype(F32)
    ahead_grad = near_grads * fac[pl.ds(me, 4)].reshape(4 * cells, ch)
    later = jnp.concatenate(
        [ahead_grad[p * cells : (p + 2) * cells].astype(BF) for p in range(3)], axis=1
    )
    grad_lat = mm(later, wc_t[...]).astype(BF)

    deep_grad = mm(grad_lat, wd_t[...])
    deep_rows = [
        jnp.concatenate(
            [
                deep_grad[frame * cells : (frame + 1) * cells, b * ch : (b + 1) * ch]
                for b in range(8)
            ],
            axis=0,
        )
        for frame in range(2)
    ]
    back = perm_v[1]
    for frame in range(2):
        ebuf[2 * frame : 2 * frame + 2, 1 : rows + 1] = (
            mm(back, (deep_rows[frame] * slopes[frame]).astype(BF))
            .astype(BF)
            .reshape(2, rows, width, ch)
        )
    hidden_grad = moved(back, deep_rows[0])

    bck = future(ebuf, 0, we_v, (0, 1, 2))
    vg_w[...] = (hidden_grad + aligned(bck)).astype(BF).reshape(vg_w.shape)
    vg_copy = give(vg_w, vg_out, 1)
    vg_copy.start()
    relay(cgr, CGR, 0)
    all_blocks(BUDDY + CGR, cgr, half_n).wait_recv()
    pre[2 : n + 2] = (cgr[0:n].astype(F32) * fac[0:n]).astype(BF)
    long = (n + 2) * cells
    coarse_rows = coarse_w.shape[0]
    piece = math.gcd(coarse_rows, ch)
    if piece % 16 == 0:
        for k in range(coarse_rows // piece):
            at = me * coarse_rows + k * piece
            left = lat_turned[pl.ds(pl.multiple_of(lax.rem(at, ch), piece), piece)]
            right = pre[pl.ds(2 - at // ch, n + 2)].reshape(long, ch)
            coarse_w[k * piece : (k + 1) * piece] = mm(left, right) * scale
    else:
        for p in range(3):
            coarse_v[pl.ds(p * ch, ch)] = (
                mm(lat_turned[...], pre[2 - p : 2 - p + n + 2].reshape(long, ch)) * scale
            )
        take_rows(coarse_v, me * coarse_rows, coarse_w)
    coarse_copy = give(coarse_w, coarse_out, 2)
    coarse_copy.start()
    later_all = jnp.concatenate([pre[2 + p : 2 + p + n].reshape(total, ch) for p in range(3)], axis=1)
    lgr[...] = mm(later_all, wc_t[...]).astype(BF).reshape(lgr.shape)

    all_blocks(STK, stk_all, n - 1).wait_recv()

    whole_v[...] = (
        mm_tn(stk_all[...].reshape(total, wb), lgr[...].reshape(total, ch)) * scale
    )
    take_rows(whole_v, mine * down_out.shape[0], down_w)
    down_copy = give(down_w, down_out, 3)
    down_copy.start()

    @pl.when(me < n - 1)
    def _():
        send_v().wait_send()
        send_w().wait_send()

    @pl.when(me > 0)
    def _():
        send_c().wait_send()
        send_n().wait_send()

    all_blocks(LAT, lat, half_n - 1).wait_send()
    all_blocks(CGR, cgr, half_n - 1).wait_send()
    all_blocks(BUDDY + LAT, lat, half_n).wait_send()
    all_blocks(BUDDY + CGR, cgr, half_n).wait_send()
    for k in (1, 2, 3):
        @pl.when(inside(-k))
        def _():
            near_send(k).wait_send()

    all_blocks(DEP, dep_all, n - 1).wait_send()
    all_blocks(STK, stk_all, n - 1).wait_send()
    for copy in (code_out_copy, vg_copy, coarse_copy, down_copy, own_copy):
        copy.wait()
    all_blocks(UPS, blocks_in, nb - 1).wait_recv()
    all_blocks(UPS, blocks_in, nb - 1).wait_send()
    if not direct:
        up_wide[...] = up_all[...].astype(F32)
        for b in range(nb):
            take_rows(up_wide.at[b], lax.rem(me * up_rows, block_rows), up_w.at[b])
        up_copy = give(up_w, up_out, 0)
        up_copy.start()
        up_copy.wait()


def tail(vg, code, down, coarse, up, vg_out, code_out, down_out, coarse_out, up_out, wide, sems):
    nb, _, wb = up.shape
    pairs = ((vg, vg_out), (code, code_out), (down, down_out), (coarse, coarse_out), (wide, up_out))
    copies = [pltpu.make_async_copy(src, dst, sems.at[k]) for k, (src, dst) in enumerate(pairs)]
    for copy in copies[:4]:
        copy.start()
    for b in range(nb):
        wide[:, b * wb : (b + 1) * wb] = up[b].astype(F32)
    copies[4].start()
    for copy in copies:
        copy.wait()


def shards(n, vf, ct, we, wd, wc, wu, wx, levels):
    frames, rows, width, ch = vf.shape
    deep = wd.shape[0]
    fine = frames * rows * width
    cells = fine // 8
    wb = max(128, deep // n)
    nb = deep // wb
    up_rows = ch // n
    block_rows = max(8, up_rows)
    scale = 1.0 / math.sqrt(n * fine)
    picks = depth_permutation(rows, width)
    perm = jnp.asarray(np.stack([picks, picks.T]), BF)
    anywhere = pl.BlockSpec(memory_space=pl.ANY)
    results = (
        (vf.shape, BF),
        ((frames // 2, rows // 2, width // 2, ch), BF),
        ((deep // n, ch), F32),
        ((wc.shape[0] // n, ch), F32),
        ((up_rows, deep), F32),
    )
    four = (4, rows + 2, width, ch)
    held_shapes = (
        results[0],
        results[1],
        results[2],
        results[3],
        ((nb, up_rows, wb), BF if block_rows == up_rows else F32),
    )
    scratch = [
        pltpu.VMEM(vf.shape, BF), pltpu.VMEM(results[1][0], BF), pltpu.VMEM(results[2][0], F32), pltpu.VMEM(results[3][0], F32),
        pltpu.VMEM((nb, up_rows, wb), F32), pltpu.VMEM((ch, (n + 2) * cells), BF),
        pltpu.VMEM(wd.shape[::-1], BF), pltpu.VMEM(wc.shape, BF),
        pltpu.VMEM((6, rows + 2, width, ch), BF), pltpu.VMEM(four, BF), pltpu.VMEM(four, BF),
        pltpu.VMEM(we.shape, BF), pltpu.VMEM(wx.shape, BF), pltpu.VMEM(wd.shape, BF),
        pltpu.VMEM(wc.shape, BF), pltpu.VMEM(wu.shape, BF), pltpu.VMEM(perm.shape, BF),
        pltpu.VMEM(levels.shape, jnp.int32),
        pltpu.VMEM((n + 5, cells, ch), BF), pltpu.VMEM((n, cells, ch), BF), pltpu.VMEM((3, cells, ch), BF),
        pltpu.VMEM((n, cells, ch), BF), pltpu.VMEM((n + 3, cells, ch), F32),
        pltpu.VMEM((n + 4, cells, ch), BF), pltpu.VMEM((n, cells, ch), BF),
        pltpu.VMEM((nb, cells, wb), BF), pltpu.VMEM((n, cells, wb), BF),
        pltpu.VMEM((nb, cells, wb), BF), pltpu.VMEM((n, cells, wb), BF),
        pltpu.VMEM((ch // block_rows, block_rows, wb), BF),
        pltpu.VMEM((nb, block_rows, wb), BF), pltpu.VMEM((nb, block_rows, wb), F32),
        pltpu.VMEM(wc.shape, F32), pltpu.VMEM((wb, ch), F32),
        pltpu.VMEM((3, fine, ch), F32), pltpu.VMEM((3, fine, ch), F32),
        pltpu.SemaphoreType.DMA((4,)), pltpu.SemaphoreType.DMA((4,)),
        pltpu.SemaphoreType.DMA((2, n // 2)), pltpu.SemaphoreType.DMA((3,)),
        pltpu.SemaphoreType.DMA((3,)), pltpu.SemaphoreType.DMA((7,)),
        pltpu.SemaphoreType.DMA((7,)), pltpu.SemaphoreType.DMA((11,)),
        pltpu.SemaphoreType.DMA((5,)),
        pltpu.SemaphoreType.REGULAR((n.bit_length() - 1,)),
    ]
    held = pl.pallas_call(
        functools.partial(kernel, n, scale),
        out_shape=tuple(pltpu.VMEM(*shape) for shape in held_shapes),
        in_specs=[anywhere] * 9,
        out_specs=(anywhere,) * 5,
        scratch_shapes=scratch,
        compiler_params=pltpu.CompilerParams(collective_id=0, has_side_effects=True),
    )(vf, ct, we, wd, wc, wu, wx, levels, perm)
    return pl.pallas_call(
        tail,
        out_shape=tuple(jax.ShapeDtypeStruct(*result) for result in results),
        in_specs=[anywhere] * 4 + [pl.BlockSpec(memory_space=pltpu.VMEM)],
        out_specs=(anywhere,) * 5,
        scratch_shapes=[pltpu.VMEM((up_rows, deep), F32), pltpu.SemaphoreType.DMA((5,))],
    )(*[pltpu.with_memory_space_constraint(part, pltpu.VMEM) for part in held])


def solution(mesh):
    placed = (P("tm", "grp", None, None), P("tm", "grp", None, None), P(), P(), P(), P(), P(), P())
    return jax.shard_map(
        functools.partial(shards, mesh.shape["tm"]),
        mesh=mesh,
        in_specs=placed,
        out_specs=(
            P("tm", "grp", None, None),
            P("tm", "grp", None, None),
            P(("grp", "tm"), None),
            P(("grp", "tm"), None),
            P(("grp", "tm"), None),
        ),
        check_vma=False,
    )
```
